16 devices in a mesh: col: 4 (over z, y), row: 4 (over x, core).
Axes of the slice: x: 2, y: 2, z: 2, core: 2. Of those that a mesh axis runs over, the one named last changes fastest.
Arguments:
- hyper_params: float32 [3], replicated
- w_in: float32 [2, 2560, 6720], P(None, 'row', 'col')
- x_in: bfloat16 [2, 2048, 2560], P(None, None, 'row')
- dy_in: bfloat16 [2, 2048, 6720], P(None, None, 'col')
- row_in: float32 [2, 2560], P(None, 'row')
- col_in: float32 [2, 6720], P(None, 'col')
- w_out: float32 [2, 6720, 2560], P(None, 'col', 'row')
- x_out: bfloat16 [2, 2048, 6720], P(None, None, 'col')
- dy_out: bfloat16 [2, 2048, 2560], P(None, None, 'row')
- row_out: float32 [2, 6720], P(None, 'col')
- col_out: float32 [2, 2560], P(None, 'row')
Outputs:
- output 1: float32 [2, 2560, 6720], P(None, 'row', 'col')
- output 2: float32 [2, 2560], P(None, 'row')
- output 3: float32 [2, 6720], P(None, 'col')
- output 4: float32 [2, 6720, 2560], P(None, 'col', 'row')
- output 5: float32 [2, 6720], P(None, 'col')
- output 6: float32 [2, 2560], P(None, 'row')
All inputs are finite; a program needn't handle non-finite values.
Results may differ from the reference program's by a relative error of at most 0.001.
Values are sent between devices in bfloat16 or wider.
A program may use at most 1 GiB of HBM per device.

```python
import jax
import jax.numpy as jnp
from jax import lax

LAYERS = 2
TOKENS = 2048
D_MODEL = 2560
D_FF = 6720
LATENT_RANK = 4
EPS_ONE = 1e-30
EPS_TWO = 1e-3
TWO_PI = 6.283185307179586


def profile(draw_key, length):
    phase_off = jax.random.uniform(draw_key, (LAYERS, LATENT_RANK, 1), jnp.float32) * TWO_PI
    freq_rank = (jnp.arange(LATENT_RANK) + 1).astype(jnp.float32)[None, :, None]
    position = (jnp.arange(length).astype(jnp.float32) / length)[None, None, :]
    return 1.0 + 0.9 * jnp.sin(TWO_PI * freq_rank * position + phase_off)


def draw_matrix(draw_key, n_rows, n_cols):
    sub_keys = jax.random.split(draw_key, 10)
    latent = jax.random.normal(sub_keys[0], (LAYERS, TOKENS, LATENT_RANK), jnp.float32)
    load_rows = jax.random.normal(sub_keys[1], (LAYERS, LATENT_RANK, n_rows), jnp.float32) * profile(sub_keys[2], n_rows)
    load_cols = jax.random.normal(sub_keys[3], (LAYERS, LATENT_RANK, n_cols), jnp.float32) * profile(sub_keys[4], n_cols)
    x_act = jnp.einsum('ltk,lkm->ltm', latent, load_rows) + jax.random.normal(sub_keys[5], (LAYERS, TOKENS, n_rows), jnp.float32)
    dy_act = (jnp.einsum('ltk,lkn->ltn', latent, load_cols) + jax.random.normal(sub_keys[6], (LAYERS, TOKENS, n_cols), jnp.float32)) / TOKENS
    w_mat = jax.random.normal(sub_keys[7], (LAYERS, n_rows, n_cols), jnp.float32) * n_rows ** -0.5
    row_stat = 6.0 * jnp.exp(0.5 * jax.random.normal(sub_keys[8], (LAYERS, n_rows), jnp.float32))
    col_stat = 6.0 * jnp.exp(0.5 * jax.random.normal(sub_keys[9], (LAYERS, n_cols), jnp.float32))
    return w_mat, x_act.astype(jnp.bfloat16), dy_act.astype(jnp.bfloat16), row_stat, col_stat


def setup_inputs(seed: int = 0) -> dict:
    sub_keys = jax.random.split(jax.random.key(seed), 3)
    low_end = jnp.array([0.5, 0.5, 0.2], dtype=jnp.float32)
    span_width = jnp.array([0.3, 0.5, 0.2], dtype=jnp.float32)
    hyper_params = low_end + span_width * jax.random.uniform(sub_keys[0], (3,), jnp.float32)
    w_in, x_in, dy_in, row_in, col_in = draw_matrix(sub_keys[1], D_MODEL, D_FF)
    w_out, x_out, dy_out, row_out, col_out = draw_matrix(sub_keys[2], D_FF, D_MODEL)
    return {'hyper_params': hyper_params, 'w_in': w_in, 'x_in': x_in, 'dy_in': dy_in, 'row_in': row_in, 'col_in': col_in, 'w_out': w_out, 'x_out': x_out, 'dy_out': dy_out, 'row_out': row_out, 'col_out': col_out}


def adafactor_one(w_mat, x_act, dy_act, row_old, col_old, hyper_params):
    beta_two = hyper_params[0]
    rho_step = hyper_params[1]
    clip_max = hyper_params[2]
    grad_mat = jnp.dot(x_act.T, dy_act, preferred_element_type=jnp.float32)
    sq_grad = grad_mat * grad_mat + EPS_ONE
    row_new = beta_two * row_old + (1.0 - beta_two) * jnp.mean(sq_grad, axis=1)
    col_new = beta_two * col_old + (1.0 - beta_two) * jnp.mean(sq_grad, axis=0)
    row_mean = jnp.mean(row_new)
    update = grad_mat * lax.rsqrt((row_new / row_mean)[:, None] * col_new[None, :])
    upd_rms = jnp.sqrt(jnp.mean(update * update))
    w_rms = jnp.sqrt(jnp.mean(w_mat * w_mat))
    step_size = rho_step * jnp.maximum(EPS_TWO, w_rms) / jnp.maximum(1.0, upd_rms / clip_max)
    return w_mat - step_size * update, row_new, col_new


def reference(hyper_params, w_in, x_in, dy_in, row_in, col_in, w_out, x_out, dy_out, row_out, col_out):
    def one_layer(layer_args):
        w_first, x_first, dy_first, row_first, col_first, w_second, x_second, dy_second, row_second, col_second = layer_args
        in_result = adafactor_one(w_first, x_first, dy_first, row_first, col_first, hyper_params)
        out_result = adafactor_one(w_second, x_second, dy_second, row_second, col_second, hyper_params)
        return in_result + out_result
    results = lax.map(one_layer, (w_in, x_in, dy_in, row_in, col_in, w_out, x_out, dy_out, row_out, col_out))
    return (results[0], results[1], results[2], results[3], results[4], results[5])
```

```python
import functools

import jax
import jax.numpy as jnp
from jax import lax
from jax.experimental import pallas as pl
from jax.experimental.pallas import tpu as pltpu
from jax.sharding import PartitionSpec as P

EPS_ONE = 1e-30
EPS_TWO = 1e-3
MESH = pl.DeviceIdType.MESH
F32 = jnp.float32
LANES = 128


def col_tiles(width):
    return [(start, min(LANES, width - start)) for start in range(0, width, LANES)]


def stats_kernel(n_col, n_row, chunk, hyper, w_in, x_in, dy_in, row_in, col_in, w_out, x_out, dy_out, row_out, col_out,
                 wv_in, row_in_new, col_in_new, wv_out, row_out_new, col_out_new,
                 upd, a_buf, b_buf, row_acc, col_acc, w_col, rx_n, rx_w, rx_s, old_n, old_w, new_narrow, new_wide,
                 a_sem, b_sem, w_sem, send_n, recv_n, send_w, recv_w, send_s, recv_s):
    n_mat, wide, narrow = upd.shape
    layers = n_mat // 2
    full_narrow, full_wide = narrow * n_row, wide * n_col
    n_total = float(full_narrow * full_wide)
    my_c, my_r = lax.axis_index("col"), lax.axis_index("row")
    n_dev = n_col * n_row
    me = my_c * n_row + my_r
    tiles = col_tiles(wide)
    nt = col_tiles(narrow)

    def loads(m, slot):
        layer = lax.rem(m, layers)

        def pair(a_src, b_src):
            return (pltpu.make_async_copy(a_src.at[layer], a_buf.at[slot], a_sem.at[slot]),
                    pltpu.make_async_copy(b_src.at[layer], b_buf.at[slot], b_sem.at[slot]))
        return pair(x_in, dy_in), pair(dy_out, x_out)

    def start_loads(m, slot):
        first, second = loads(m, slot)

        @pl.when(m < layers)
        def _():
            for copy in first:
                copy.start()

        @pl.when(m >= layers)
        def _():
            for copy in second:
                copy.start()

    start_loads(jnp.int32(0), 0)
    barrier = pltpu.get_barrier_semaphore()
    for d in range(1, n_dev):
        peer = lax.rem(me + d, n_dev)
        pl.semaphore_signal(barrier, inc=1, device_id=(peer // n_row, lax.rem(peer, n_row)), device_id_type=MESH)

    old_n[...] = jnp.zeros_like(old_n)
    old_w[...] = jnp.zeros_like(old_w)
    for m in range(n_mat):
        rx_n[m, my_c] = jnp.zeros(rx_n.shape[2:], F32)
        rx_w[m, my_r] = jnp.zeros(rx_w.shape[2:], F32)
    for layer in range(layers):
        for m, src_n, src_w in ((layer, row_in, col_in), (layers + layer, col_out, row_out)):
            for j, (s, w) in enumerate(nt):
                old_n[m, j:j + 1, :w] = src_n[layer:layer + 1, s:s + w]
            for j, (s, w) in enumerate(tiles):
                old_w[m, j:j + 1, :w] = src_w[layer:layer + 1, s:s + w]
    pl.semaphore_wait(barrier, n_dev - 1)

    w_copies = ([pltpu.make_async_copy(w_in.at[i], wv_in.at[i], w_sem.at[i]) for i in range(layers)]
                + [pltpu.make_async_copy(w_out.at[i], wv_out.at[i], w_sem.at[layers + i]) for i in range(layers)])

    def on_weights(m, fn):
        @pl.when(m < layers)
        def _():
            fn(wv_in)

        @pl.when(m >= layers)
        def _():
            fn(wv_out)

    def narrow_copy(m, d):
        peer = lax.rem(my_c + d, n_col)
        return pltpu.make_async_remote_copy(
            src_ref=rx_n.at[m, my_c], dst_ref=rx_n.at[m, my_c], send_sem=send_n.at[m, d], recv_sem=recv_n.at[m, my_c],
            device_id=(peer, my_r), device_id_type=MESH)

    def narrow_arrival(m, d):
        src = lax.rem(my_c + d, n_col)
        return pltpu.make_async_remote_copy(
            src_ref=rx_n.at[m, src], dst_ref=rx_n.at[m, src], send_sem=send_n.at[m, d], recv_sem=recv_n.at[m, src],
            device_id=(src, my_r), device_id_type=MESH)

    def wide_copy(m, d):
        peer = lax.rem(my_r + d, n_row)
        return pltpu.make_async_remote_copy(
            src_ref=rx_w.at[m, my_r], dst_ref=rx_w.at[m, my_r], send_sem=send_w.at[m, d], recv_sem=recv_w.at[m, my_r],
            device_id=(my_c, peer), device_id_type=MESH)

    def wide_arrival(m, d):
        src = lax.rem(my_r + d, n_row)
        return pltpu.make_async_remote_copy(
            src_ref=rx_w.at[m, src], dst_ref=rx_w.at[m, src], send_sem=send_w.at[m, d], recv_sem=recv_w.at[m, src],
            device_id=(my_c, src), device_id_type=MESH)

    def scalar_copy(m, d):
        peer = lax.rem(me + d, n_dev)
        return pltpu.make_async_remote_copy(
            src_ref=rx_s.at[m, me], dst_ref=rx_s.at[m, me], send_sem=send_s.at[m, d], recv_sem=recv_s.at[m, me],
            device_id=(peer // n_row, lax.rem(peer, n_row)), device_id_type=MESH)

    def scalar_arrival(m, d):
        src = lax.rem(me + d, n_dev)
        return pltpu.make_async_remote_copy(
            src_ref=rx_s.at[m, src], dst_ref=rx_s.at[m, src], send_sem=send_s.at[m, d], recv_sem=recv_s.at[m, src],
            device_id=(src // n_row, lax.rem(src, n_row)), device_id_type=MESH)

    def products(m):
        slot = lax.rem(m, 2)
        for copy in loads(m, slot)[0]:
            copy.wait()

        @pl.when(m + 1 < n_mat)
        def _():
            start_loads(m + 1, 1 - slot)

        for i in range(n_mat):
            @pl.when(m == i)
            def _():
                w_copies[i].start()

        total = jnp.zeros((8, narrow), F32)
        for s in range(0, wide, chunk):
            g = jnp.dot(b_buf[slot, s:s + chunk, :], a_buf[slot], preferred_element_type=F32)
            upd[m, s:s + chunk, :] = g
            q = g * g
            part = q[:, :LANES]
            for t, tw in nt[1:]:
                part = part + q[:, t:t + tw]
            row_acc[s:s + chunk, :] = part
            total = total + jnp.sum(q.reshape(chunk // 8, 8, narrow), axis=0)
        sums = jnp.sum(total, axis=0, keepdims=True)
        for j, (t, tw) in enumerate(nt):
            rx_n[m, my_c, j:j + 1, :] = sums[:, t:t + tw]
        for d in range(1, n_col):
            narrow_copy(m, d).start()
        for j, (t, tw) in enumerate(tiles):
            block = row_acc[t:t + tw, :].T
            rx_w[m, my_r, j:j + 1, :tw] = jnp.sum(block, axis=0, keepdims=True)
        for d in range(1, n_row):
            wide_copy(m, d).start()

    lane = lax.broadcasted_iota(jnp.int32, (1, LANES), 1)

    def second_moments(m):
        beta = hyper[0]
        layer = lax.rem(m, layers)
        is_in = m < layers
        for d in range(1, n_col):
            narrow_arrival(m, d).wait_recv()
        for d in range(1, n_row):
            wide_arrival(m, d).wait_recv()
        sum_n = rx_n[m, 0]
        for src in range(1, n_col):
            sum_n = sum_n + rx_n[m, src]
        sum_w = rx_w[m, 0]
        for src in range(1, n_row):
            sum_w = sum_w + rx_w[m, src]
        new_n = beta * old_n[m] + (1.0 - beta) * (sum_n / full_wide + EPS_ONE)
        new_w = beta * old_w[m] + (1.0 - beta) * (sum_w / full_narrow + EPS_ONE)
        new_narrow[m] = new_n
        new_wide[m] = new_w

        def block_mean(v, length):
            index = (lax.broadcasted_iota(jnp.int32, v.shape, 0) * LANES + lax.broadcasted_iota(jnp.int32, v.shape, 1))
            masked = jnp.where(index < length, v, 0.0)
            return jnp.sum(jnp.sum(masked, axis=0, keepdims=True), axis=1, keepdims=True) / length

        mean_row = jnp.where(is_in, block_mean(new_n, narrow), block_mean(new_w, wide))
        one = jnp.ones_like(mean_row)
        inv_n = lax.rsqrt(new_n / jnp.where(is_in, mean_row, one))
        inv_w = lax.rsqrt(new_w / jnp.where(is_in, one, mean_row))
        for j, (t, tw) in enumerate(tiles):
            w_col[t:t + tw, :] = jnp.broadcast_to(inv_w[j:j + 1, :tw], (LANES, tw)).T
        inv_rows = [jnp.broadcast_to(inv_n[j:j + 1, :], (8, LANES)) for j in range(len(nt))]

        def scale(i, acc):
            rows = pl.ds(pl.multiple_of(i * 8, 8), 8)
            a = w_col[rows, :]
            for j, (t, tw) in enumerate(nt):
                u = upd[m, rows, t:t + tw] * a * inv_rows[j]
                upd[m, rows, t:t + tw] = u
                acc = acc + u * u
            return acc

        total = jnp.sum(lax.fori_loop(0, wide // 8, scale, jnp.zeros((8, LANES), F32), unroll=6), keepdims=True)

        def send(wv):
            def square(i, acc):
                rows = pl.ds(pl.multiple_of(i * 8, 8), 8)
                for t, tw in nt:
                    v = wv[layer, rows, t:t + tw]
                    acc = acc + v * v
                return acc

            w_sq = jnp.sum(lax.fori_loop(0, wide // 8, square, jnp.zeros((8, LANES), F32), unroll=6), keepdims=True)
            rx_s[m, me] = jnp.where(lane < 32, total, jnp.where(lane < 64, w_sq, mean_row))

        on_weights(m, send)
        for d in range(1, n_dev):
            scalar_copy(m, d).start()

    def step_factor(m):
        for d in range(1, n_dev):
            scalar_arrival(m, d).wait_recv()
        got = [rx_s[m, src] for src in range(n_dev)]
        mean = got[0]
        for v in got[1:]:
            mean = mean + v
        s_full = jnp.sum(jnp.where(lane == 64, mean, 0.0), axis=1, keepdims=True) / n_dev
        own = jnp.sum(jnp.where(lane == 64, rx_s[m, me], 0.0), axis=1, keepdims=True)
        acc = None
        for v in got:
            ratio = s_full / pltpu.roll(v, 64, 1)
            term = v * jnp.where(lane < 32, ratio, 1.0)
            acc = term if acc is None else acc + term
        upd_sq = jnp.sum(jnp.where(lane == 0, acc, 0.0), axis=1, keepdims=True)
        w_sq = jnp.sum(jnp.where(lane == 32, acc, 0.0), axis=1, keepdims=True)
        upd_rms = jnp.sqrt(upd_sq / n_total)
        w_rms = jnp.sqrt(w_sq / n_total)
        size = hyper[1] * jnp.maximum(EPS_TWO, w_rms) / jnp.maximum(1.0, upd_rms / hyper[2])
        k = jnp.broadcast_to(size * jnp.sqrt(s_full / own), (8, LANES))
        layer = lax.rem(m, layers)

        def apply(wv):
            def update(i, carry):
                rows = pl.ds(pl.multiple_of(i * 8, 8), 8)
                for t, tw in nt:
                    wv[layer, rows, t:t + tw] = wv[layer, rows, t:t + tw] - k * upd[m, rows, t:t + tw]
                return carry
            lax.fori_loop(0, wide // 8, update, 0, unroll=6)

        on_weights(m, apply)

    def body(i, _):
        @pl.when(i < n_mat)
        def _():
            products(i)

        for m in range(n_mat):
            @pl.when(i == m + 1)
            def _(m=m):
                w_copies[m].wait()

        @pl.when(jnp.logical_and(i >= 1, i <= n_mat))
        def _():
            second_moments(i - 1)

        @pl.when(i >= 2)
        def _():
            step_factor(i - 2)
        return 0

    lax.fori_loop(0, n_mat + 2, body, 0)

    def drain(m, _):
        for d in range(1, n_col):
            narrow_copy(m, d).wait_send()
        for d in range(1, n_row):
            wide_copy(m, d).wait_send()
        for d in range(1, n_dev):
            scalar_copy(m, d).wait_send()
        return 0

    lax.fori_loop(0, n_mat, drain, 0)
    for layer in range(layers):
        for m, dst_n, dst_w in ((layer, row_in_new, col_in_new), (layers + layer, col_out_new, row_out_new)):
            for j, (s, w) in enumerate(nt):
                dst_n[layer:layer + 1, s:s + w] = new_narrow[m, j:j + 1, :w]
            for j, (s, w) in enumerate(tiles):
                dst_w[layer:layer + 1, s:s + w] = new_wide[m, j:j + 1, :w]


def write_kernel(*refs):
    count = (len(refs) - 1) // 2
    srcs, dsts, sem = refs[:count], refs[count:2 * count], refs[-1]
    copies = [pltpu.make_async_copy(src, dst, sem.at[i]) for i, (src, dst) in enumerate(zip(srcs, dsts))]
    for copy in copies:
        copy.start()
    for copy in copies:
        copy.wait()


def solution(mesh):
    n_col = mesh.shape['col']
    n_row = mesh.shape['row']
    tile_in = P(None, 'row', 'col')
    tile_out = P(None, 'col', 'row')
    lane_row = P(None, None, 'row')
    lane_col = P(None, None, 'col')
    vec_row = P(None, 'row')
    vec_col = P(None, 'col')

    def local_step(hyper_params, w_in, x_in, dy_in, row_in, col_in, w_out, x_out, dy_out, row_out, col_out):
        layers, narrow, wide = w_in.shape
        tokens = x_in.shape[1]
        n_mat = 2 * layers
        n_dev = n_col * n_row
        hbm = pl.BlockSpec(memory_space=pltpu.HBM)
        vmem = pl.BlockSpec(memory_space=pltpu.VMEM)
        smem = pl.BlockSpec(memory_space=pltpu.SMEM)
        dma = pltpu.SemaphoreType.DMA
        nr, wr = 8, 16
        swap = lambda v: jnp.swapaxes(v, 1, 2)
        chunk = 336
        shapes = [v.shape for v in (w_out, row_in, col_in, w_out, row_out, col_out)]
        results = pl.pallas_call(
            functools.partial(stats_kernel, n_col, n_row, chunk),
            out_shape=tuple(pltpu.VMEM(shape, F32) for shape in shapes),
            in_specs=[smem, hbm, hbm, hbm, vmem, vmem, hbm, hbm, hbm, vmem, vmem],
            out_specs=(vmem,) * 6,
            scratch_shapes=[
                pltpu.VMEM((n_mat, wide, narrow), F32),
                pltpu.VMEM((2, tokens, narrow), jnp.bfloat16),
                pltpu.VMEM((2, wide, tokens), jnp.bfloat16),
                pltpu.VMEM((wide, LANES), F32),
                pltpu.VMEM((8, narrow), F32),
                pltpu.VMEM((wide, LANES), F32),
                pltpu.VMEM((n_mat, n_col, nr, LANES), F32),
                pltpu.VMEM((n_mat, n_row, wr, LANES), F32),
                pltpu.VMEM((n_mat, n_dev, 1, LANES), F32),
                pltpu.VMEM((n_mat, nr, LANES), F32),
                pltpu.VMEM((n_mat, wr, LANES), F32),
                pltpu.VMEM((n_mat, nr, LANES), F32),
                pltpu.VMEM((n_mat, wr, LANES), F32),
                dma((2,)), dma((2,)), dma((n_mat,)),
                dma((n_mat, n_col)), dma((n_mat, n_col)),
                dma((n_mat, n_row)), dma((n_mat, n_row)),
                dma((n_mat, n_dev)), dma((n_mat, n_dev)),
            ],
            compiler_params=pltpu.CompilerParams(collective_id=0, has_side_effects=True, vmem_limit_bytes=44 << 20),
            name="stats",
        )(hyper_params, swap(w_in), x_in, swap(dy_in), row_in, col_in, w_out, swap(x_out), dy_out, row_out, col_out)
        w_in_new, row_in_new, col_in_new, w_out_new, row_out_new, col_out_new = pl.pallas_call(
            write_kernel,
            out_shape=tuple(pltpu.HBM(shape, F32) for shape in shapes),
            in_specs=[vmem] * 6,
            out_specs=(hbm,) * 6,
            scratch_shapes=[dma((6,))],
            compiler_params=pltpu.CompilerParams(vmem_limit_bytes=1 << 20),
            name="write",
        )(*(pltpu.with_memory_space_constraint(v, pltpu.VMEM) for v in results))
        return swap(w_in_new), row_in_new, col_in_new, w_out_new, row_out_new, col_out_new

    return jax.shard_map(local_step, mesh=mesh, in_specs=(P(), tile_in, lane_row, lane_col, vec_row, vec_col, tile_out, lane_col, lane_row, vec_col, vec_row), out_specs=(tile_in, vec_row, vec_col, tile_out, vec_col, vec_row), check_vma=False)
```

```python
import functools

import jax
import jax.numpy as jnp
from jax import lax
from jax.experimental import pallas as pl
from jax.experimental.pallas import tpu as pltpu
from jax.sharding import PartitionSpec as P

EPS_ONE = 1e-30
EPS_TWO = 1e-3
MESH = pl.DeviceIdType.MESH
F32 = jnp.float32
LANES = 128


def col_tiles(width):
    return [(start, min(LANES, width - start)) for start in range(0, width, LANES)]


def stats_kernel(n_col, n_row, chunk, hyper, w_in, x_in, dy_in, row_in, col_in, w_out, x_out, dy_out, row_out, col_out,
                 wv_in, row_in_new, col_in_new, wv_out, row_out_new, col_out_new,
                 upd, a_buf, b_buf, row_acc, w_col, inv_n, rx_n, rx_w, rx_s, old_n, old_w,
                 a_sem, b_sem, w_sem, send_n, recv_n, send_w, recv_w, send_s, recv_s):
    n_mat, wide, narrow = upd.shape
    layers = n_mat // 2
    full_narrow, full_wide = narrow * n_row, wide * n_col
    n_total = float(full_narrow * full_wide)
    my_c, my_r = lax.axis_index("col"), lax.axis_index("row")
    n_dev = n_col * n_row
    me = my_c * n_row + my_r
    tiles = col_tiles(wide)
    nt = col_tiles(narrow)

    order = [(s, chunk) for s in range(0, wide, chunk)]

    def loads(m):
        slot, layer = m % 2, m % layers
        a_src, b_src = (x_in, dy_in) if m < layers else (dy_out, x_out)
        return ([pltpu.make_async_copy(a_src.at[layer], a_buf.at[slot], a_sem.at[slot])]
                + [pltpu.make_async_copy(b_src.at[layer, pl.ds(s, w)], b_buf.at[slot, pl.ds(s, w)], b_sem.at[slot, i])
                   for i, (s, w) in enumerate(order)])

    for copy in loads(0):
        copy.start()
    barrier = pltpu.get_barrier_semaphore()
    for d in range(1, n_dev):
        peer = lax.rem(me + d, n_dev)
        pl.semaphore_signal(barrier, inc=1, device_id=(peer // n_row, lax.rem(peer, n_row)), device_id_type=MESH)

    old_n[...] = jnp.zeros_like(old_n)
    old_w[...] = jnp.zeros_like(old_w)
    for m in range(n_mat):
        rx_n[m, my_c] = jnp.zeros(rx_n.shape[2:], F32)
        rx_w[m, my_r] = jnp.zeros(rx_w.shape[2:], F32)
    for layer in range(layers):
        for m, src_n, src_w in ((layer, row_in, col_in), (layers + layer, col_out, row_out)):
            for j, (s, w) in enumerate(nt):
                old_n[m, j:j + 1, :w] = src_n[layer:layer + 1, s:s + w]
            for j, (s, w) in enumerate(tiles):
                old_w[m, j:j + 1, :w] = src_w[layer:layer + 1, s:s + w]

    w_copies = ([pltpu.make_async_copy(w_in.at[i], wv_in.at[i], w_sem.at[i]) for i in range(layers)]
                + [pltpu.make_async_copy(w_out.at[i], wv_out.at[i], w_sem.at[layers + i]) for i in range(layers)])

    def weights(m):
        return wv_in.at[m % layers] if m < layers else wv_out.at[m % layers]

    def narrow_copy(m, d):
        peer = lax.rem(my_c + d, n_col)
        return pltpu.make_async_remote_copy(
            src_ref=rx_n.at[m, my_c], dst_ref=rx_n.at[m, my_c], send_sem=send_n.at[m, d], recv_sem=recv_n.at[m, my_c],
            device_id=(peer, my_r), device_id_type=MESH)

    def narrow_arrival(m, d):
        src = lax.rem(my_c + d, n_col)
        return pltpu.make_async_remote_copy(
            src_ref=rx_n.at[m, src], dst_ref=rx_n.at[m, src], send_sem=send_n.at[m, d], recv_sem=recv_n.at[m, src],
            device_id=(src, my_r), device_id_type=MESH)

    def wide_copy(m, d):
        peer = lax.rem(my_r + d, n_row)
        return pltpu.make_async_remote_copy(
            src_ref=rx_w.at[m, my_r], dst_ref=rx_w.at[m, my_r], send_sem=send_w.at[m, d], recv_sem=recv_w.at[m, my_r],
            device_id=(my_c, peer), device_id_type=MESH)

    def wide_arrival(m, d):
        src = lax.rem(my_r + d, n_row)
        return pltpu.make_async_remote_copy(
            src_ref=rx_w.at[m, src], dst_ref=rx_w.at[m, src], send_sem=send_w.at[m, d], recv_sem=recv_w.at[m, src],
            device_id=(my_c, src), device_id_type=MESH)

    def scalar_copy(m, d):
        peer = lax.rem(me + d, n_dev)
        return pltpu.make_async_remote_copy(
            src_ref=rx_s.at[m, me], dst_ref=rx_s.at[m, me], send_sem=send_s.at[m, d], recv_sem=recv_s.at[m, me],
            device_id=(peer // n_row, lax.rem(peer, n_row)), device_id_type=MESH)

    def scalar_arrival(m, d):
        src = lax.rem(me + d, n_dev)
        return pltpu.make_async_remote_copy(
            src_ref=rx_s.at[m, src], dst_ref=rx_s.at[m, src], send_sem=send_s.at[m, d], recv_sem=recv_s.at[m, src],
            device_id=(src // n_row, lax.rem(src, n_row)), device_id_type=MESH)

    lane = lax.broadcasted_iota(jnp.int32, (1, LANES), 1)
    zero = jnp.zeros((8, LANES), F32)
    sq_sum = {}
    norm_sum = {}
    row_mean = {}

    def fold(v):
        return jnp.sum(v.reshape(v.shape[0] // 8, 8, v.shape[1]), axis=0)

    def scale_rows(m, s, w):
        acc = norm_sum.get(m, zero)
        a = w_col[m % 2, s:s + w, :]
        for j, (t, tw) in enumerate(nt):
            u = upd[m, s:s + w, t:t + tw] * a * inv_n[m, j:j + 1, :]
            upd[m, s:s + w, t:t + tw] = u
            acc = acc + fold(u * u)
        norm_sum[m] = acc

    def square_rows(m, s, w):
        acc = sq_sum.get(m, zero)
        for t, tw in nt:
            v = weights(m)[s:s + w, t:t + tw]
            acc = acc + fold(v * v)
        sq_sum[m] = acc

    def products(m, blocks, total, beside):
        slot = m % 2
        for s, w in blocks:
            g = jnp.dot(b_buf[slot, s:s + w, :], a_buf[slot], preferred_element_type=F32)
            upd[m, s:s + w, :] = g
            q = g * g
            part = q[:, :LANES]
            for t, tw in nt[1:]:
                part = part + q[:, t:t + tw]
            total = total + fold(q)
            row_acc[s:s + w, :] = part
            for t, tw in tiles:
                if s < t + tw <= s + w:
                    block = row_acc[t:t + tw, :].T
                    j = t // LANES
                    rx_w[m, my_r, j:j + 1, :tw] = jnp.sum(block, axis=0, keepdims=True)
            for fn in beside:
                fn(s, w)
        return total

    def send_moments(m, total):
        sums = jnp.sum(total, axis=0, keepdims=True)
        for j, (t, tw) in enumerate(nt):
            rx_n[m, my_c, j:j + 1, :] = sums[:, t:t + tw]
        for d in range(1, n_col):
            narrow_copy(m, d).start()
        for d in range(1, n_row):
            wide_copy(m, d).start()

    def wait_moments(m):
        for d in range(1, n_col):
            narrow_arrival(m, d).wait_recv()
        for d in range(1, n_row):
            wide_arrival(m, d).wait_recv()

    def second_moments(m):
        beta = hyper[0]
        layer = m % layers
        sum_n = rx_n[m, 0]
        for src in range(1, n_col):
            sum_n = sum_n + rx_n[m, src]
        sum_w = rx_w[m, 0]
        for src in range(1, n_row):
            sum_w = sum_w + rx_w[m, src]
        new_n = beta * old_n[m] + (1.0 - beta) * (sum_n / full_wide + EPS_ONE)
        new_w = beta * old_w[m] + (1.0 - beta) * (sum_w / full_narrow + EPS_ONE)
        dst_n, dst_w = (row_in_new, col_in_new) if m < layers else (col_out_new, row_out_new)
        for j, (t, tw) in enumerate(nt):
            dst_n[layer:layer + 1, t:t + tw] = new_n[j:j + 1, :tw]
        for j, (t, tw) in enumerate(tiles):
            dst_w[layer:layer + 1, t:t + tw] = new_w[j:j + 1, :tw]
        v, length = (new_n, narrow) if m < layers else (new_w, wide)
        index = lax.broadcasted_iota(jnp.int32, v.shape, 0) * LANES + lax.broadcasted_iota(jnp.int32, v.shape, 1)
        mean = jnp.sum(jnp.sum(jnp.where(index < length, v, 0.0), axis=0, keepdims=True), axis=1, keepdims=True) / length
        row_mean[m] = mean
        scaled_n, scaled_w = (new_n / mean, new_w) if m < layers else (new_n, new_w / mean)
        inv_n[m] = lax.rsqrt(scaled_n)
        inv_w = lax.rsqrt(scaled_w)
        for j, (t, tw) in enumerate(tiles):
            w_col[m % 2, t:t + tw, :] = jnp.broadcast_to(inv_w[j:j + 1, :tw], (LANES, tw)).T

    def each_peer(fn):
        def body(d, carry):
            fn(d)
            return carry
        lax.fori_loop(1, n_dev, body, 0)

    def send_scalars(m):
        norm = jnp.sum(norm_sum[m], keepdims=True)
        w_sq = jnp.sum(sq_sum[m], keepdims=True)
        rx_s[m, me] = jnp.where(lane < 32, norm, jnp.where(lane < 64, w_sq, row_mean[m]))
        each_peer(lambda d: scalar_copy(m, d).start())

    def step_factor(m):
        each_peer(lambda d: scalar_arrival(m, d).wait_recv())
        got = rx_s[m]
        s_full = jnp.sum(jnp.where(lane == 64, jnp.sum(got, axis=0), 0.0), axis=1, keepdims=True) / n_dev
        own = jnp.sum(jnp.where(lane == 64, rx_s[m, me], 0.0), axis=1, keepdims=True)
        ratio = s_full[None] / pltpu.roll(got, 64, 2)
        acc = jnp.sum(got * jnp.where(lane[None] < 32, ratio, 1.0), axis=0)
        upd_sq = jnp.sum(jnp.where(lane == 0, acc, 0.0), axis=1, keepdims=True)
        w_sq = jnp.sum(jnp.where(lane == 32, acc, 0.0), axis=1, keepdims=True)
        upd_rms = jnp.sqrt(upd_sq / n_total)
        w_rms = jnp.sqrt(w_sq / n_total)
        size = hyper[1] * jnp.maximum(EPS_TWO, w_rms) / jnp.maximum(1.0, upd_rms / hyper[2])
        return jnp.broadcast_to(size * jnp.sqrt(s_full / own), (8, LANES))

    def update(m):
        k = step_factor(m)
        w_ref = weights(m)

        def body(i, carry):
            rows = pl.ds(pl.multiple_of(i * 8, 8), 8)
            for t, tw in nt:
                w_ref[rows, t:t + tw] = w_ref[rows, t:t + tw] - k * upd[m, rows, t:t + tw]
            return carry
        lax.fori_loop(0, wide // 8, body, 0, unroll=6)

    last = n_mat - 1
    for m in range(n_mat):
        total = jnp.zeros((8, narrow), F32)
        copies = loads(m)
        blocks = order
        if m == 0:
            for copy in copies[:2]:
                copy.wait()
            for copy in loads(1):
                copy.start()
            total = products(m, order[:1], total, [])
            blocks, copies = order[1:], copies[2:]
        for copy in copies:
            copy.wait()
        if 1 <= m < last:
            for copy in loads(m + 1):
                copy.start()
        w_copies[m].start()
        beside = []
        if m >= 1:
            w_copies[m - 1].wait()
            beside.append(functools.partial(square_rows, m - 1))
        if m >= 2:
            wait_moments(m - 2)
            second_moments(m - 2)
            beside.append(functools.partial(scale_rows, m - 2))
        total = products(m, blocks, total, beside)
        if m == 0:
            pl.semaphore_wait(barrier, n_dev - 1)
        send_moments(m, total)
        if m >= 2:
            send_scalars(m - 2)

    w_copies[last].wait()
    wait_moments(last - 1)
    second_moments(last - 1)
    for s, w in order:
        scale_rows(last - 1, s, w)
    send_scalars(last - 1)
    for s, w in order:
        square_rows(last, s, w)
    for m in range(last - 2):
        update(m)
    wait_moments(last)
    second_moments(last)
    for s, w in order:
        scale_rows(last, s, w)
    send_scalars(last)
    for m in range(last - 2, last):
        update(m)
    update(last)

    def drain(m, _):
        for d in range(1, n_col):
            narrow_copy(m, d).wait_send()
        for d in range(1, n_row):
            wide_copy(m, d).wait_send()
        for d in range(1, n_dev):
            scalar_copy(m, d).wait_send()
        return 0

    lax.fori_loop(0, n_mat, drain, 0)


def write_kernel(*refs):
    count = (len(refs) - 1) // 2
    srcs, dsts, sem = refs[:count], refs[count:2 * count], refs[-1]
    copies = [pltpu.make_async_copy(src, dst, sem.at[i]) for i, (src, dst) in enumerate(zip(srcs, dsts))]
    for copy in copies:
        copy.start()
    for copy in copies:
        copy.wait()


def solution(mesh):
    n_col = mesh.shape['col']
    n_row = mesh.shape['row']
    tile_in = P(None, 'row', 'col')
    tile_out = P(None, 'col', 'row')
    lane_row = P(None, None, 'row')
    lane_col = P(None, None, 'col')
    vec_row = P(None, 'row')
    vec_col = P(None, 'col')

    def local_step(hyper_params, w_in, x_in, dy_in, row_in, col_in, w_out, x_out, dy_out, row_out, col_out):
        layers, narrow, wide = w_in.shape
        tokens = x_in.shape[1]
        n_mat = 2 * layers
        n_dev = n_col * n_row
        hbm = pl.BlockSpec(memory_space=pltpu.HBM)
        vmem = pl.BlockSpec(memory_space=pltpu.VMEM)
        smem = pl.BlockSpec(memory_space=pltpu.SMEM)
        dma = pltpu.SemaphoreType.DMA
        nr, wr = 8, 16
        swap = lambda v: jnp.swapaxes(v, 1, 2)
        chunk = 336
        shapes = [v.shape for v in (w_out, row_in, col_in, w_out, row_out, col_out)]
        results = pl.pallas_call(
            functools.partial(stats_kernel, n_col, n_row, chunk),
            out_shape=tuple(pltpu.VMEM(shape, F32) for shape in shapes),
            in_specs=[smem, hbm, hbm, hbm, vmem, vmem, hbm, hbm, hbm, vmem, vmem],
            out_specs=(vmem,) * 6,
            scratch_shapes=[
                pltpu.VMEM((n_mat, wide, narrow), F32),
                pltpu.VMEM((2, tokens, narrow), jnp.bfloat16),
                pltpu.VMEM((2, wide, tokens), jnp.bfloat16),
                pltpu.VMEM((wide, LANES), F32),
                pltpu.VMEM((2, wide, LANES), F32),
                pltpu.VMEM((n_mat, nr, LANES), F32),
                pltpu.VMEM((n_mat, n_col, nr, LANES), F32),
                pltpu.VMEM((n_mat, n_row, wr, LANES), F32),
                pltpu.VMEM((n_mat, n_dev, 1, LANES), F32),
                pltpu.VMEM((n_mat, nr, LANES), F32),
                pltpu.VMEM((n_mat, wr, LANES), F32),
                dma((2,)), dma((2, wide // chunk)), dma((n_mat,)),
                dma((n_mat, n_col)), dma((n_mat, n_col)),
                dma((n_mat, n_row)), dma((n_mat, n_row)),
                dma((n_mat, n_dev)), dma((n_mat, n_dev)),
            ],
            compiler_params=pltpu.CompilerParams(collective_id=0, has_side_effects=True, vmem_limit_bytes=44 << 20),
            name="stats",
        )(hyper_params, swap(w_in), x_in, swap(dy_in), row_in, col_in, w_out, swap(x_out), dy_out, row_out, col_out)
        w_in_new, row_in_new, col_in_new, w_out_new, row_out_new, col_out_new = pl.pallas_call(
            write_kernel,
            out_shape=tuple(pltpu.HBM(shape, F32) for shape in shapes),
            in_specs=[vmem] * 6,
            out_specs=(hbm,) * 6,
            scratch_shapes=[dma((6,))],
            compiler_params=pltpu.CompilerParams(vmem_limit_bytes=1 << 20),
            name="write",
        )(*(pltpu.with_memory_space_constraint(v, pltpu.VMEM) for v in results))
        return swap(w_in_new), row_in_new, col_in_new, w_out_new, row_out_new, col_out_new

    return jax.shard_map(local_step, mesh=mesh, in_specs=(P(), tile_in, lane_row, lane_col, vec_row, vec_col, tile_out, lane_col, lane_row, vec_col, vec_row), out_specs=(tile_in, vec_row, vec_col, tile_out, vec_col, vec_row), check_vma=False)
```

```python
import functools

import jax
import jax.numpy as jnp
from jax import lax
from jax.experimental import pallas as pl
from jax.experimental.pallas import tpu as pltpu
from jax.sharding import PartitionSpec as P

EPS_ONE = 1e-30
EPS_TWO = 1e-3
MESH = pl.DeviceIdType.MESH
F32 = jnp.float32
LANES = 128


def col_tiles(width):
    return [(start, min(LANES, width - start)) for start in range(0, width, LANES)]


def stats_kernel(n_col, n_row, sizes, hyper, w_in, x_in, dy_in, row_in, col_in, w_out, x_out, dy_out, row_out, col_out,
                 wv_in, row_in_new, col_in_new, wv_out, row_out_new, col_out_new,
                 upd, a_buf, b_buf, row_acc, w_col, inv_n, rx_n, rx_w, rx_s, old_n, old_w,
                 a_sem, b_sem, w_sem, send_n, recv_n, send_w, recv_w, send_s, recv_s):
    n_mat, wide, narrow = upd.shape
    layers = n_mat // 2
    full_narrow, full_wide = narrow * n_row, wide * n_col
    n_total = float(full_narrow * full_wide)
    my_c, my_r = lax.axis_index("col"), lax.axis_index("row")
    n_dev = n_col * n_row
    me = my_c * n_row + my_r
    tiles = col_tiles(wide)
    nt = col_tiles(narrow)

    def split(start, *lengths):
        return [(start + sum(lengths[:i]), w) for i, w in enumerate(lengths)]

    order = split(0, *sizes)

    def loads(m):
        slot, layer = m % 2, m % layers
        a_src, b_src = (x_in, dy_in) if m < layers else (dy_out, x_out)
        return ([pltpu.make_async_copy(a_src.at[layer], a_buf.at[slot], a_sem.at[slot])]
                + [pltpu.make_async_copy(b_src.at[layer, pl.ds(s, w)], b_buf.at[slot, pl.ds(s, w)], b_sem.at[slot, i])
                   for i, (s, w) in enumerate(order)])

    for copy in loads(0):
        copy.start()
    barrier = pltpu.get_barrier_semaphore()
    for d in range(1, n_dev):
        peer = lax.rem(me + d, n_dev)
        pl.semaphore_signal(barrier, inc=1, device_id=(peer // n_row, lax.rem(peer, n_row)), device_id_type=MESH)

    old_n[...] = jnp.zeros_like(old_n)
    old_w[...] = jnp.zeros_like(old_w)
    for m in range(n_mat):
        rx_n[m, my_c] = jnp.zeros(rx_n.shape[2:], F32)
        rx_w[m, my_r] = jnp.zeros(rx_w.shape[2:], F32)
    for layer in range(layers):
        for m, src_n, src_w in ((layer, row_in, col_in), (layers + layer, col_out, row_out)):
            for j, (s, w) in enumerate(nt):
                old_n[m, j:j + 1, :w] = src_n[layer:layer + 1, s:s + w]
            for j, (s, w) in enumerate(tiles):
                old_w[m, j:j + 1, :w] = src_w[layer:layer + 1, s:s + w]

    w_copies = ([pltpu.make_async_copy(w_in.at[i], wv_in.at[i], w_sem.at[i]) for i in range(layers)]
                + [pltpu.make_async_copy(w_out.at[i], wv_out.at[i], w_sem.at[layers + i]) for i in range(layers)])

    def weights(m):
        return wv_in.at[m % layers] if m < layers else wv_out.at[m % layers]

    def narrow_copy(m, d):
        peer = lax.rem(my_c + d, n_col)
        return pltpu.make_async_remote_copy(
            src_ref=rx_n.at[m, my_c], dst_ref=rx_n.at[m, my_c], send_sem=send_n.at[m, d], recv_sem=recv_n.at[m, my_c],
            device_id=(peer, my_r), device_id_type=MESH)

    def narrow_arrival(m, d):
        src = lax.rem(my_c + d, n_col)
        return pltpu.make_async_remote_copy(
            src_ref=rx_n.at[m, src], dst_ref=rx_n.at[m, src], send_sem=send_n.at[m, d], recv_sem=recv_n.at[m, src],
            device_id=(src, my_r), device_id_type=MESH)

    def wide_copy(m, d):
        peer = lax.rem(my_r + d, n_row)
        return pltpu.make_async_remote_copy(
            src_ref=rx_w.at[m, my_r], dst_ref=rx_w.at[m, my_r], send_sem=send_w.at[m, d], recv_sem=recv_w.at[m, my_r],
            device_id=(my_c, peer), device_id_type=MESH)

    def wide_arrival(m, d):
        src = lax.rem(my_r + d, n_row)
        return pltpu.make_async_remote_copy(
            src_ref=rx_w.at[m, src], dst_ref=rx_w.at[m, src], send_sem=send_w.at[m, d], recv_sem=recv_w.at[m, src],
            device_id=(my_c, src), device_id_type=MESH)

    def scalar_copy(m, d):
        peer = lax.rem(me + d, n_dev)
        return pltpu.make_async_remote_copy(
            src_ref=rx_s.at[m, me], dst_ref=rx_s.at[m, me], send_sem=send_s.at[m, d], recv_sem=recv_s.at[m, me],
            device_id=(peer // n_row, lax.rem(peer, n_row)), device_id_type=MESH)

    def scalar_arrival(m, d):
        src = lax.rem(me + d, n_dev)
        return pltpu.make_async_remote_copy(
            src_ref=rx_s.at[m, src], dst_ref=rx_s.at[m, src], send_sem=send_s.at[m, d], recv_sem=recv_s.at[m, src],
            device_id=(src // n_row, lax.rem(src, n_row)), device_id_type=MESH)

    lane = lax.broadcasted_iota(jnp.int32, (1, LANES), 1)
    zero = jnp.zeros((8, narrow), F32)
    sq_sum = {}
    norm_sum = {}
    row_mean = {}

    group = 16

    def fold(v):
        return sum(v[r:r + 8] for r in range(8, v.shape[0], 8)) + v[:8]

    def scale_group(m, rows, acc):
        a = jnp.concatenate([w_col[m % 2, rows, :]] * len(nt), axis=1)
        u = upd[m, rows, :] * a * inv_n[m % 2]
        upd[m, rows, :] = u
        return acc + fold(u * u)

    def square_group(m, rows, acc):
        v = weights(m)[rows, :]
        return acc + fold(v * v)

    def all_rows(fn, sums, m):
        sums[m] = lax.fori_loop(0, wide // group, lambda i, acc: fn(m, pl.ds(pl.multiple_of(i * group, group), group), acc),
                                zero, unroll=5)

    def products(m, blocks, total):
        slot = m % 2
        for s, w in blocks:
            g = jnp.dot(b_buf[slot, s:s + w, :], a_buf[slot], preferred_element_type=F32)
            upd[m, s:s + w, :] = g
            q = g * g
            part = q[:, :LANES]
            for t, tw in nt[1:]:
                part = part + q[:, t:t + tw]
            total = total + jnp.sum(q.reshape(w // 8, 8, narrow), axis=0)
            row_acc[s:s + w, :] = part
            for t, tw in tiles:
                if s < t + tw <= s + w:
                    block = row_acc[t:t + tw, :].T
                    j = t // LANES
                    rx_w[m, my_r, j:j + 1, :tw] = jnp.sum(block, axis=0, keepdims=True)
        return total

    def send_moments(m, total):
        sums = jnp.sum(total, axis=0, keepdims=True)
        for j, (t, tw) in enumerate(nt):
            rx_n[m, my_c, j:j + 1, :] = sums[:, t:t + tw]
        for d in range(1, n_col):
            narrow_copy(m, d).start()
        for d in range(1, n_row):
            wide_copy(m, d).start()

    def wait_moments(m):
        for d in range(1, n_col):
            narrow_arrival(m, d).wait_recv()
        for d in range(1, n_row):
            wide_arrival(m, d).wait_recv()

    def second_moments(m):
        beta = hyper[0]
        layer = m % layers
        sum_n = rx_n[m, 0]
        for src in range(1, n_col):
            sum_n = sum_n + rx_n[m, src]
        sum_w = rx_w[m, 0]
        for src in range(1, n_row):
            sum_w = sum_w + rx_w[m, src]
        new_n = beta * old_n[m] + (1.0 - beta) * (sum_n / full_wide + EPS_ONE)
        new_w = beta * old_w[m] + (1.0 - beta) * (sum_w / full_narrow + EPS_ONE)
        dst_n, dst_w = (row_in_new, col_in_new) if m < layers else (col_out_new, row_out_new)
        for j, (t, tw) in enumerate(nt):
            dst_n[layer:layer + 1, t:t + tw] = new_n[j:j + 1, :tw]
        for j, (t, tw) in enumerate(tiles):
            dst_w[layer:layer + 1, t:t + tw] = new_w[j:j + 1, :tw]
        v, length = (new_n, narrow) if m < layers else (new_w, wide)
        index = lax.broadcasted_iota(jnp.int32, v.shape, 0) * LANES + lax.broadcasted_iota(jnp.int32, v.shape, 1)
        mean = jnp.sum(jnp.sum(jnp.where(index < length, v, 0.0), axis=0, keepdims=True), axis=1, keepdims=True) / length
        row_mean[m] = mean
        root = jnp.sqrt(mean)
        scaled = lax.rsqrt(new_n) * root
        for j, (t, tw) in enumerate(nt):
            inv_n[m % 2, :, t:t + tw] = scaled[j:j + 1, :]
        inv_w = lax.rsqrt(new_w)
        for j, (t, tw) in enumerate(tiles):
            w_col[m % 2, t:t + tw, :] = jnp.broadcast_to(inv_w[j:j + 1, :tw], (LANES, tw)).T

    def each_peer(fn):
        def body(d, carry):
            fn(d)
            return carry
        lax.fori_loop(1, n_dev, body, 0)

    def send_scalars(m):
        norm = jnp.sum(norm_sum[m], keepdims=True)
        w_sq = jnp.sum(sq_sum[m], keepdims=True)
        rx_s[m, me] = jnp.where(lane < 32, norm, jnp.where(lane < 64, w_sq, row_mean[m]))
        each_peer(lambda d: scalar_copy(m, d).start())

    def step_factor(m):
        each_peer(lambda d: scalar_arrival(m, d).wait_recv())
        got = rx_s[m]
        s_full = jnp.sum(jnp.where(lane == 64, jnp.sum(got, axis=0), 0.0), axis=1, keepdims=True) / n_dev
        own = jnp.sum(jnp.where(lane == 64, rx_s[m, me], 0.0), axis=1, keepdims=True)
        ratio = s_full[None] / pltpu.roll(got, 64, 2)
        acc = jnp.sum(got * jnp.where(lane[None] < 32, ratio, 1.0), axis=0)
        upd_sq = jnp.sum(jnp.where(lane == 0, acc, 0.0), axis=1, keepdims=True)
        w_sq = jnp.sum(jnp.where(lane == 32, acc, 0.0), axis=1, keepdims=True)
        upd_rms = jnp.sqrt(upd_sq / n_total)
        w_rms = jnp.sqrt(w_sq / n_total)
        size = hyper[1] * jnp.maximum(EPS_TWO, w_rms) / jnp.maximum(1.0, upd_rms / hyper[2])
        return size * jnp.sqrt(s_full / own)

    def update(m):
        k = step_factor(m)
        w_ref = weights(m)

        def body(i, carry):
            rows = pl.ds(pl.multiple_of(i * group, group), group)
            w_ref[rows, :] = w_ref[rows, :] - k * upd[m, rows, :]
            return carry
        lax.fori_loop(0, wide // group, body, 0, unroll=5)

    last = n_mat - 1
    for m in range(n_mat):
        total = zero
        copies = loads(m)
        blocks = order
        if m == 0:
            for copy in copies[:2]:
                copy.wait()
            for copy in loads(1):
                copy.start()
            total = products(m, split(0, 208, 224), total)
            blocks, copies = order[1:-1] + split(order[-1][0], 208, 208), copies[2:]
        for copy in copies:
            copy.wait()
        if 1 <= m < last:
            for copy in loads(m + 1):
                copy.start()
        w_copies[m].start()
        total = products(m, blocks, total)
        if m == 0:
            pl.semaphore_wait(barrier, n_dev - 1)
        send_moments(m, total)

    for m in range(n_mat):
        w_copies[m].wait()
        all_rows(square_group, sq_sum, m)
    for m in range(n_mat):
        wait_moments(m)
        second_moments(m)
        all_rows(scale_group, norm_sum, m)
        send_scalars(m)
    for m in range(n_mat):
        update(m)

    def drain(m, _):
        for d in range(1, n_col):
            narrow_copy(m, d).wait_send()
        for d in range(1, n_row):
            wide_copy(m, d).wait_send()
        for d in range(1, n_dev):
            scalar_copy(m, d).wait_send()
        return 0

    lax.fori_loop(0, n_mat, drain, 0)


def write_kernel(*refs):
    count = (len(refs) - 1) // 2
    srcs, dsts, sem = refs[:count], refs[count:2 * count], refs[-1]
    copies = [pltpu.make_async_copy(src, dst, sem.at[i]) for i, (src, dst) in enumerate(zip(srcs, dsts))]
    for copy in copies:
        copy.start()
    for copy in copies:
        copy.wait()


def solution(mesh):
    n_col = mesh.shape['col']
    n_row = mesh.shape['row']
    tile_in = P(None, 'row', 'col')
    tile_out = P(None, 'col', 'row')
    lane_row = P(None, None, 'row')
    lane_col = P(None, None, 'col')
    vec_row = P(None, 'row')
    vec_col = P(None, 'col')

    def local_step(hyper_params, w_in, x_in, dy_in, row_in, col_in, w_out, x_out, dy_out, row_out, col_out):
        layers, narrow, wide = w_in.shape
        tokens = x_in.shape[1]
        n_mat = 2 * layers
        n_dev = n_col * n_row
        hbm = pl.BlockSpec(memory_space=pltpu.HBM)
        vmem = pl.BlockSpec(memory_space=pltpu.VMEM)
        smem = pl.BlockSpec(memory_space=pltpu.SMEM)
        dma = pltpu.SemaphoreType.DMA
        nr, wr = 8, 16
        swap = lambda v: jnp.swapaxes(v, 1, 2)
        sizes = (432, 416, 416, 416)
        shapes = [v.shape for v in (w_out, row_in, col_in, w_out, row_out, col_out)]
        results = pl.pallas_call(
            functools.partial(stats_kernel, n_col, n_row, sizes),
            out_shape=tuple(pltpu.VMEM(shape, F32) for shape in shapes),
            in_specs=[smem, hbm, hbm, hbm, vmem, vmem, hbm, hbm, hbm, vmem, vmem],
            out_specs=(vmem,) * 6,
            scratch_shapes=[
                pltpu.VMEM((n_mat, wide, narrow), F32),
                pltpu.VMEM((2, tokens, narrow), jnp.bfloat16),
                pltpu.VMEM((2, wide, tokens), jnp.bfloat16),
                pltpu.VMEM((wide, LANES), F32),
                pltpu.VMEM((2, wide, LANES), F32),
                pltpu.VMEM((2, 1, narrow), F32),
                pltpu.VMEM((n_mat, n_col, nr, LANES), F32),
                pltpu.VMEM((n_mat, n_row, wr, LANES), F32),
                pltpu.VMEM((n_mat, n_dev, 1, LANES), F32),
                pltpu.VMEM((n_mat, nr, LANES), F32),
                pltpu.VMEM((n_mat, wr, LANES), F32),
                dma((2,)), dma((2, len(sizes))), dma((n_mat,)),
                dma((n_mat, n_col)), dma((n_mat, n_col)),
                dma((n_mat, n_row)), dma((n_mat, n_row)),
                dma((n_mat, n_dev)), dma((n_mat, n_dev)),
            ],
            compiler_params=pltpu.CompilerParams(collective_id=0, has_side_effects=True, vmem_limit_bytes=44 << 20),
            name="stats",
        )(hyper_params, swap(w_in), x_in, swap(dy_in), row_in, col_in, w_out, swap(x_out), dy_out, row_out, col_out)
        w_in_new, row_in_new, col_in_new, w_out_new, row_out_new, col_out_new = pl.pallas_call(
            write_kernel,
            out_shape=tuple(pltpu.HBM(shape, F32) for shape in shapes),
            in_specs=[vmem] * 6,
            out_specs=(hbm,) * 6,
            scratch_shapes=[dma((6,))],
            compiler_params=pltpu.CompilerParams(vmem_limit_bytes=1 << 20),
            name="write",
        )(*(pltpu.with_memory_space_constraint(v, pltpu.VMEM) for v in results))
        return swap(w_in_new), row_in_new, col_in_new, w_out_new, row_out_new, col_out_new

    return jax.shard_map(local_step, mesh=mesh, in_specs=(P(), tile_in, lane_row, lane_col, vec_row, vec_col, tile_out, lane_col, lane_row, vec_col, vec_row), out_specs=(tile_in, vec_row, vec_col, tile_out, vec_col, vec_row), check_vma=False)
```

```python
import functools

import jax
import jax.numpy as jnp
from jax import lax
from jax.experimental import pallas as pl
from jax.experimental.pallas import tpu as pltpu
from jax.sharding import PartitionSpec as P

EPS_ONE = 1e-30
EPS_TWO = 1e-3
MESH = pl.DeviceIdType.MESH
F32 = jnp.float32
LANES = 128


def col_tiles(width):
    return [(start, min(LANES, width - start)) for start in range(0, width, LANES)]


def stats_kernel(n_col, n_row, sizes, hyper, w_in, x_in, dy_in, row_in, col_in, w_out, x_out, dy_out, row_out, col_out,
                 wv_in, row_in_new, col_in_new, wv_out, row_out_new, col_out_new,
                 upd, a_buf, b_buf, row_acc, w_col, inv_n, rx_n, rx_w, rx_a, rx_b, old_n, old_w,
                 a_sem, b_sem, w_sem, send_n, recv_n, send_w, recv_w, send_s, recv_s):
    n_mat, wide, narrow = upd.shape
    layers = n_mat // 2
    full_narrow, full_wide = narrow * n_row, wide * n_col
    n_total = float(full_narrow * full_wide)
    my_c, my_r = lax.axis_index("col"), lax.axis_index("row")
    n_dev = n_col * n_row
    me = my_c * n_row + my_r
    tiles = col_tiles(wide)
    nt = col_tiles(narrow)

    def split(start, *lengths):
        return [(start + sum(lengths[:i]), w) for i, w in enumerate(lengths)]

    order = split(0, *sizes)

    def loads(m):
        slot, layer = m % 2, m % layers
        a_src, b_src = (x_in, dy_in) if m < layers else (dy_out, x_out)
        return ([pltpu.make_async_copy(a_src.at[layer], a_buf.at[slot], a_sem.at[slot])]
                + [pltpu.make_async_copy(b_src.at[layer, pl.ds(s, w)], b_buf.at[slot, pl.ds(s, w)], b_sem.at[slot, i])
                   for i, (s, w) in enumerate(order)])

    for copy in loads(0):
        copy.start()
    barrier = pltpu.get_barrier_semaphore()
    peers_c = [lax.rem(my_c + d, n_col) for d in range(n_col)]
    peers_r = [lax.rem(my_r + d, n_row) for d in range(n_row)]
    peers = [(c, r) for i, c in enumerate(peers_c) for j, r in enumerate(peers_r) if i or j]
    for peer in peers:
        pl.semaphore_signal(barrier, inc=1, device_id=peer, device_id_type=MESH)

    old_n[...] = jnp.zeros_like(old_n)
    old_w[...] = jnp.zeros_like(old_w)
    for m in range(n_mat):
        rx_n[m, my_c] = jnp.zeros(rx_n.shape[2:], F32)
        rx_w[m, my_r] = jnp.zeros(rx_w.shape[2:], F32)
    for layer in range(layers):
        for m, src_n, src_w in ((layer, row_in, col_in), (layers + layer, col_out, row_out)):
            for j, (s, w) in enumerate(nt):
                old_n[m, j:j + 1, :w] = src_n[layer:layer + 1, s:s + w]
            for j, (s, w) in enumerate(tiles):
                old_w[m, j:j + 1, :w] = src_w[layer:layer + 1, s:s + w]

    w_copies = ([pltpu.make_async_copy(w_in.at[i], wv_in.at[i], w_sem.at[i]) for i in range(layers)]
                + [pltpu.make_async_copy(w_out.at[i], wv_out.at[i], w_sem.at[layers + i]) for i in range(layers)])

    def weights(m):
        return wv_in.at[m % layers] if m < layers else wv_out.at[m % layers]

    def send(buf, index, send_sem, recv_sem, peer):
        pltpu.make_async_remote_copy(src_ref=buf.at[index], dst_ref=buf.at[index], send_sem=send_sem, recv_sem=recv_sem,
                                     device_id=peer, device_id_type=MESH).start()

    def wait_bytes(ref, sem):
        pltpu.make_async_copy(ref, ref, sem).wait()

    lane = lax.broadcasted_iota(jnp.int32, (1, LANES), 1)
    zero = jnp.zeros((8, narrow), F32)
    sq_sum = {}
    row_mean = {}

    group = 16

    def scale_group(m, rows, acc):
        u = upd[m, rows, :] * jnp.concatenate([w_col[m, rows, :]] * len(nt), axis=1)
        upd[m, rows, :] = u
        return acc + u * u

    def square_group(m, rows, acc):
        v = weights(m)[rows, :]
        return acc + v * v

    def all_rows(fn, m):
        return lax.fori_loop(0, wide // group,
                             lambda i, acc: fn(m, pl.ds(pl.multiple_of(i * group, group), group), acc),
                             jnp.zeros((group, narrow), F32), unroll=21)

    def products(m, blocks, total, square=None):
        slot = m % 2
        for s, w in blocks:
            g = jnp.dot(b_buf[slot, s:s + w, :], a_buf[slot], preferred_element_type=F32)
            upd[m, s:s + w, :] = g
            q = g * g
            part = q[:, :LANES]
            for t, tw in nt[1:]:
                part = part + q[:, t:t + tw]
            total = total + jnp.sum(q.reshape(w // 8, 8, narrow), axis=0)
            row_acc[s:s + w, :] = part
            if square is not None:
                acc = sq_sum.get(square, jnp.zeros((group, narrow), F32))
                for r in range(s, s + w, group):
                    acc = square_group(square, pl.ds(r, group), acc)
                sq_sum[square] = acc
            for t, tw in tiles:
                if s < t + tw <= s + w:
                    block = row_acc[t:t + tw, :].T
                    j = t // LANES
                    rx_w[m, my_r, j:j + 1, :tw] = jnp.sum(block, axis=0, keepdims=True)
        return total

    def send_moments(m, total):
        sums = jnp.sum(total, axis=0, keepdims=True)
        for j, (t, tw) in enumerate(nt):
            rx_n[m, my_c, j:j + 1, :] = sums[:, t:t + tw]
        for c in peers_c[1:]:
            send(rx_n.at[m], my_c, send_n.at[m], recv_n.at[m], (c, my_r))
        for r in peers_r[1:]:
            send(rx_w.at[m], my_r, send_w.at[m], recv_w.at[m], (my_c, r))

    def wait_moments(m):
        wait_bytes(rx_n.at[m, pl.ds(0, n_col - 1)], recv_n.at[m])
        wait_bytes(rx_w.at[m, pl.ds(0, n_row - 1)], recv_w.at[m])

    def second_moments(m):
        beta = hyper[0]
        layer = m % layers
        sum_n = rx_n[m, 0]
        for src in range(1, n_col):
            sum_n = sum_n + rx_n[m, src]
        sum_w = rx_w[m, 0]
        for src in range(1, n_row):
            sum_w = sum_w + rx_w[m, src]
        new_n = beta * old_n[m] + (1.0 - beta) * (sum_n / full_wide + EPS_ONE)
        new_w = beta * old_w[m] + (1.0 - beta) * (sum_w / full_narrow + EPS_ONE)
        dst_n, dst_w = (row_in_new, col_in_new) if m < layers else (col_out_new, row_out_new)
        for j, (t, tw) in enumerate(nt):
            dst_n[layer:layer + 1, t:t + tw] = new_n[j:j + 1, :tw]
        for j, (t, tw) in enumerate(tiles):
            dst_w[layer:layer + 1, t:t + tw] = new_w[j:j + 1, :tw]
        v, length = (new_n, narrow) if m < layers else (new_w, wide)
        index = lax.broadcasted_iota(jnp.int32, v.shape, 0) * LANES + lax.broadcasted_iota(jnp.int32, v.shape, 1)
        mean = jnp.sum(jnp.sum(jnp.where(index < length, v, 0.0), axis=0, keepdims=True), axis=1, keepdims=True) / length
        row_mean[m] = mean
        root = jnp.sqrt(mean)
        scaled = lax.rsqrt(new_n) * root
        for j, (t, tw) in enumerate(nt):
            inv_n[m, :, t:t + tw] = scaled[j:j + 1, :]
        inv_w = lax.rsqrt(new_w)
        for j, (t, tw) in enumerate(tiles):
            w_col[m, t:t + tw, :] = jnp.broadcast_to(inv_w[j:j + 1, :tw], (LANES, tw)).T

    def send_scalars(group_of, buf, i):
        for slot, m in enumerate(group_of):
            norm = jnp.sum(all_rows(scale_group, m), axis=0, keepdims=True) * inv_n[m] * inv_n[m]
            norm = jnp.sum(norm, axis=1, keepdims=True)
            w_sq = jnp.sum(jnp.sum(sq_sum[m], axis=0, keepdims=True), axis=1, keepdims=True)
            buf[me, slot] = jnp.where(lane < 32, norm, jnp.where(lane < 64, w_sq, row_mean[m]))
        for peer in peers:
            send(buf, me, send_s.at[i], recv_s.at[i], peer)

    def step_factor(buf, slot):
        got = buf[:, slot]
        s_full = jnp.sum(jnp.where(lane == 64, jnp.sum(got, axis=0), 0.0), axis=1, keepdims=True) / n_dev
        own = jnp.sum(jnp.where(lane == 64, buf[me, slot], 0.0), axis=1, keepdims=True)
        ratio = s_full[None] / pltpu.roll(got, 64, 2)
        acc = jnp.sum(got * jnp.where(lane[None] < 32, ratio, 1.0), axis=0)
        upd_sq = jnp.sum(jnp.where(lane == 0, acc, 0.0), axis=1, keepdims=True)
        w_sq = jnp.sum(jnp.where(lane == 32, acc, 0.0), axis=1, keepdims=True)
        upd_rms = jnp.sqrt(upd_sq / n_total)
        w_rms = jnp.sqrt(w_sq / n_total)
        size = hyper[1] * jnp.maximum(EPS_TWO, w_rms) / jnp.maximum(1.0, upd_rms / hyper[2])
        return size * jnp.sqrt(s_full / own)

    def update(group_of, buf, i):
        wait_bytes(buf.at[pl.ds(0, n_dev - 1)], recv_s.at[i])
        factors = [step_factor(buf, slot) * inv_n[m] for slot, m in enumerate(group_of)]
        for m, k in zip(group_of, factors):
            w_ref = weights(m)
            k = jnp.broadcast_to(k, (8, narrow))
            k = jnp.concatenate([k] * (group // 8), axis=0)

            def body(step, carry, m=m, w_ref=w_ref, k=k):
                rows = pl.ds(pl.multiple_of(step * group, group), group)
                w_ref[rows, :] = w_ref[rows, :] - k * upd[m, rows, :]
                return carry
            lax.fori_loop(0, wide // group, body, 0, unroll=21)

    last = n_mat - 1
    for m in range(n_mat):
        total = zero
        copies = loads(m)
        blocks = order
        if m == 0:
            for copy in copies[:2]:
                copy.wait()
            for copy in loads(1):
                copy.start()
            total = products(m, split(0, 208, 224), total)
            blocks, copies = order[1:-1] + split(order[-1][0], 208, 208), copies[2:]
        for copy in copies:
            copy.wait()
        if 1 <= m < last:
            for copy in loads(m + 1):
                copy.start()
        w_copies[m].start()
        if m:
            w_copies[m - 1].wait()
        if m >= 2:
            wait_moments(m - 2)
            second_moments(m - 2)
        total = products(m, blocks, total, m - 1 if m else None)
        if m == 0:
            pl.semaphore_wait(barrier, n_dev - 1)
        send_moments(m, total)

    early, late = list(range(last)), [last]
    wait_moments(last - 1)
    second_moments(last - 1)
    send_scalars(early, rx_a, 0)
    w_copies[last].wait()
    sq_sum[last] = all_rows(square_group, last)
    wait_moments(last)
    second_moments(last)
    send_scalars(late, rx_b, 1)
    update(early, rx_a, 0)
    for m in range(n_mat):
        wait_bytes(rx_n.at[m, pl.ds(0, n_col - 1)], send_n.at[m])
        wait_bytes(rx_w.at[m, pl.ds(0, n_row - 1)], send_w.at[m])
    wait_bytes(rx_a.at[pl.ds(0, n_dev - 1)], send_s.at[0])
    wait_bytes(rx_b.at[pl.ds(0, n_dev - 1)], send_s.at[1])
    update(late, rx_b, 1)


def write_kernel(*refs):
    count = (len(refs) - 1) // 2
    srcs, dsts, sem = refs[:count], refs[count:2 * count], refs[-1]
    copies = []
    for src, dst in zip(srcs, dsts):
        if len(src.shape) == 2:
            pieces = [(src, dst)]
        else:
            rows = src.shape[1] // 2
            pieces = [(src.at[i, pl.ds(r, rows)], dst.at[i, pl.ds(r, rows)])
                      for i in range(src.shape[0]) for r in (0, rows)]
        for src_piece, dst_piece in pieces:
            copies.append(pltpu.make_async_copy(src_piece, dst_piece, sem.at[len(copies)]))
    for copy in copies:
        copy.start()
    for copy in copies:
        copy.wait()


def solution(mesh):
    n_col = mesh.shape['col']
    n_row = mesh.shape['row']
    tile_in = P(None, 'row', 'col')
    tile_out = P(None, 'col', 'row')
    lane_row = P(None, None, 'row')
    lane_col = P(None, None, 'col')
    vec_row = P(None, 'row')
    vec_col = P(None, 'col')

    def local_step(hyper_params, w_in, x_in, dy_in, row_in, col_in, w_out, x_out, dy_out, row_out, col_out):
        layers, narrow, wide = w_in.shape
        tokens = x_in.shape[1]
        n_mat = 2 * layers
        n_dev = n_col * n_row
        hbm = pl.BlockSpec(memory_space=pltpu.HBM)
        vmem = pl.BlockSpec(memory_space=pltpu.VMEM)
        smem = pl.BlockSpec(memory_space=pltpu.SMEM)
        dma = pltpu.SemaphoreType.DMA
        nr, wr = 8, 16
        swap = lambda v: jnp.swapaxes(v, 1, 2)
        sizes = (432, 416, 416, 416)
        shapes = [v.shape for v in (w_out, row_in, col_in, w_out, row_out, col_out)]
        results = pl.pallas_call(
            functools.partial(stats_kernel, n_col, n_row, sizes),
            out_shape=tuple(pltpu.VMEM(shape, F32) for shape in shapes),
            in_specs=[smem, hbm, hbm, hbm, vmem, vmem, hbm, hbm, hbm, vmem, vmem],
            out_specs=(vmem,) * 6,
            scratch_shapes=[
                pltpu.VMEM((n_mat, wide, narrow), F32),
                pltpu.VMEM((2, tokens, narrow), jnp.bfloat16),
                pltpu.VMEM((2, wide, tokens), jnp.bfloat16),
                pltpu.VMEM((wide, LANES), F32),
                pltpu.VMEM((n_mat, wide, LANES), F32),
                pltpu.VMEM((n_mat, 1, narrow), F32),
                pltpu.VMEM((n_mat, n_col, nr, LANES), F32),
                pltpu.VMEM((n_mat, n_row, wr, LANES), F32),
                pltpu.VMEM((n_dev, n_mat - 1, 1, LANES), F32),
                pltpu.VMEM((n_dev, 1, 1, LANES), F32),
                pltpu.VMEM((n_mat, nr, LANES), F32),
                pltpu.VMEM((n_mat, wr, LANES), F32),
                dma((2,)), dma((2, len(sizes))), dma((n_mat,)),
                dma((n_mat,)), dma((n_mat,)), dma((n_mat,)), dma((n_mat,)), dma((2,)), dma((2,)),
            ],
            compiler_params=pltpu.CompilerParams(collective_id=0, has_side_effects=True, vmem_limit_bytes=44 << 20),
            name="stats",
        )(hyper_params, swap(w_in), x_in, swap(dy_in), row_in, col_in, w_out, swap(x_out), dy_out, row_out, col_out)
        w_in_new, row_in_new, col_in_new, w_out_new, row_out_new, col_out_new = pl.pallas_call(
            write_kernel,
            out_shape=tuple(pltpu.HBM(shape, F32) for shape in shapes),
            in_specs=[vmem] * 6,
            out_specs=(hbm,) * 6,
            scratch_shapes=[dma((8 * layers + 4,))],
            compiler_params=pltpu.CompilerParams(vmem_limit_bytes=1 << 20),
            name="write",
        )(*(pltpu.with_memory_space_constraint(v, pltpu.VMEM) for v in results))
        return swap(w_in_new), row_in_new, col_in_new, w_out_new, row_out_new, col_out_new

    return jax.shard_map(local_step, mesh=mesh, in_specs=(P(), tile_in, lane_row, lane_col, vec_row, vec_col, tile_out, lane_col, lane_row, vec_col, vec_row), out_specs=(tile_in, vec_row, vec_col, tile_out, vec_col, vec_row), check_vma=False)
```

```python
import functools

import jax
import jax.numpy as jnp
from jax import lax
from jax.experimental import pallas as pl
from jax.experimental.pallas import tpu as pltpu
from jax.sharding import PartitionSpec as P

EPS_ONE = 1e-30
EPS_TWO = 1e-3
MESH = pl.DeviceIdType.MESH
F32 = jnp.float32
LANES = 128


def col_tiles(width):
    return [(start, min(LANES, width - start)) for start in range(0, width, LANES)]


def stats_kernel(n_col, n_row, sizes, hyper, w_in, x_in, dy_in, row_in, col_in, w_out, x_out, dy_out, row_out, col_out,
                 wv_in, row_in_new, col_in_new, wv_out, row_out_new, col_out_new,
                 upd, a_buf, b_buf, row_acc, w_col, inv_n, rx_n, rx_w, rx_a, rx_b, old_n, old_w,
                 a_sem, b_sem, w_sem, send_n, recv_n, send_w, recv_w, send_s, recv_s):
    n_mat, wide, narrow = upd.shape
    layers = n_mat // 2
    full_narrow, full_wide = narrow * n_row, wide * n_col
    n_total = float(full_narrow * full_wide)
    my_c, my_r = lax.axis_index("col"), lax.axis_index("row")
    n_dev = n_col * n_row
    me = my_c * n_row + my_r
    tiles = col_tiles(wide)
    nt = col_tiles(narrow)

    def split(start, *lengths):
        return [(start + sum(lengths[:i]), w) for i, w in enumerate(lengths)]

    order = split(0, *sizes)

    def loads(m):
        slot, layer = m % 2, m % layers
        a_src, b_src = (x_in, dy_in) if m < layers else (dy_out, x_out)
        return ([pltpu.make_async_copy(a_src.at[layer], a_buf.at[slot], a_sem.at[slot])]
                + [pltpu.make_async_copy(b_src.at[layer, pl.ds(s, w)], b_buf.at[slot, pl.ds(s, w)], b_sem.at[slot, i])
                   for i, (s, w) in enumerate(order)])

    for copy in loads(0):
        copy.start()
    barrier = pltpu.get_barrier_semaphore()
    peers_c = [lax.rem(my_c + d, n_col) for d in range(n_col)]
    peers_r = [lax.rem(my_r + d, n_row) for d in range(n_row)]
    peers = [(c, r) for i, c in enumerate(peers_c) for j, r in enumerate(peers_r) if i or j]
    for peer in peers:
        pl.semaphore_signal(barrier, inc=1, device_id=peer, device_id_type=MESH)

    old_n[...] = jnp.zeros_like(old_n)
    old_w[...] = jnp.zeros_like(old_w)
    for m in range(n_mat):
        rx_n[m, my_c] = jnp.zeros(rx_n.shape[2:], F32)
        rx_w[m, my_r] = jnp.zeros(rx_w.shape[2:], F32)
    for layer in range(layers):
        for m, src_n, src_w in ((layer, row_in, col_in), (layers + layer, col_out, row_out)):
            for j, (s, w) in enumerate(nt):
                old_n[m, j:j + 1, :w] = src_n[layer:layer + 1, s:s + w]
            for j, (s, w) in enumerate(tiles):
                old_w[m, j:j + 1, :w] = src_w[layer:layer + 1, s:s + w]

    w_copies = ([pltpu.make_async_copy(w_in.at[i], wv_in.at[i], w_sem.at[i]) for i in range(layers)]
                + [pltpu.make_async_copy(w_out.at[i], wv_out.at[i], w_sem.at[layers + i]) for i in range(layers)])

    def weights(m):
        return wv_in.at[m % layers] if m < layers else wv_out.at[m % layers]

    def send(buf, index, send_sem, recv_sem, peer):
        pltpu.make_async_remote_copy(src_ref=buf.at[index], dst_ref=buf.at[index], send_sem=send_sem, recv_sem=recv_sem,
                                     device_id=peer, device_id_type=MESH).start()

    def wait_bytes(ref, sem):
        pltpu.make_async_copy(ref, ref, sem).wait()

    lane = lax.broadcasted_iota(jnp.int32, (1, LANES), 1)
    zero = jnp.zeros((8, narrow), F32)
    zeros = jnp.zeros((16, narrow), F32)
    sq_sum = {}
    row_mean = {}

    group, stretch = 16, 336

    def scale_group(m, at, r, acc):
        rows = slice(r, r + group)
        g = at(upd.at[m])
        u = g[rows, :] * jnp.concatenate([at(w_col.at[m])[rows, :]] * len(nt), axis=1)
        g[rows, :] = u
        return acc + u * u

    def square_group(m, at, r, acc):
        v = at(weights(m))[r:r + group, :]
        return acc + v * v

    def all_rows(fn, init):
        def body(i, carry):
            at = lambda ref: ref.at[pl.ds(pl.multiple_of(i * stretch, stretch), stretch)]
            for r in range(0, stretch, group):
                carry = fn(at, r, carry)
            return carry
        return lax.fori_loop(0, wide // stretch, body, init)

    def products(m, blocks, total, square=None):
        slot = m % 2
        for s, w in blocks:
            g = jnp.dot(b_buf[slot, s:s + w, :], a_buf[slot], preferred_element_type=F32)
            upd[m, s:s + w, :] = g
            q = g * g
            part = q[:, :LANES]
            for t, tw in nt[1:]:
                part = part + q[:, t:t + tw]
            total = total + jnp.sum(q.reshape(w // 8, 8, narrow), axis=0)
            row_acc[s:s + w, :] = part
            if square is not None:
                acc = sq_sum.get(square, zeros)
                for r in range(s, s + w, group):
                    acc = square_group(square, lambda ref: ref, r, acc)
                sq_sum[square] = acc
            for t, tw in tiles:
                if s < t + tw <= s + w:
                    block = row_acc[t:t + tw, :].T
                    j = t // LANES
                    rx_w[m, my_r, j:j + 1, :tw] = jnp.sum(block, axis=0, keepdims=True)
        return total

    def send_moments(m, total):
        sums = jnp.sum(total, axis=0, keepdims=True)
        for j, (t, tw) in enumerate(nt):
            rx_n[m, my_c, j:j + 1, :] = sums[:, t:t + tw]
        for c in peers_c[1:]:
            send(rx_n.at[m], my_c, send_n.at[m], recv_n.at[m], (c, my_r))
        for r in peers_r[1:]:
            send(rx_w.at[m], my_r, send_w.at[m], recv_w.at[m], (my_c, r))

    def wait_moments(m):
        wait_bytes(rx_n.at[m, pl.ds(0, n_col - 1)], recv_n.at[m])
        wait_bytes(rx_w.at[m, pl.ds(0, n_row - 1)], recv_w.at[m])

    def second_moments(m):
        beta = hyper[0]
        layer = m % layers
        sum_n = rx_n[m, 0]
        for src in range(1, n_col):
            sum_n = sum_n + rx_n[m, src]
        sum_w = rx_w[m, 0]
        for src in range(1, n_row):
            sum_w = sum_w + rx_w[m, src]
        new_n = beta * old_n[m] + (1.0 - beta) * (sum_n / full_wide + EPS_ONE)
        new_w = beta * old_w[m] + (1.0 - beta) * (sum_w / full_narrow + EPS_ONE)
        dst_n, dst_w = (row_in_new, col_in_new) if m < layers else (col_out_new, row_out_new)
        for j, (t, tw) in enumerate(nt):
            dst_n[layer:layer + 1, t:t + tw] = new_n[j:j + 1, :tw]
        for j, (t, tw) in enumerate(tiles):
            dst_w[layer:layer + 1, t:t + tw] = new_w[j:j + 1, :tw]
        v, length = (new_n, narrow) if m < layers else (new_w, wide)
        index = lax.broadcasted_iota(jnp.int32, v.shape, 0) * LANES + lax.broadcasted_iota(jnp.int32, v.shape, 1)
        mean = jnp.sum(jnp.sum(jnp.where(index < length, v, 0.0), axis=0, keepdims=True), axis=1, keepdims=True) / length
        row_mean[m] = mean
        root = jnp.sqrt(mean)
        scaled = lax.rsqrt(new_n) * root
        for j, (t, tw) in enumerate(nt):
            inv_n[m, :, t:t + tw] = scaled[j:j + 1, :]
        inv_w = lax.rsqrt(new_w)
        for j, (t, tw) in enumerate(tiles):
            w_col[m, t:t + tw, :] = jnp.broadcast_to(inv_w[j:j + 1, :tw], (LANES, tw)).T

    def send_scalars(group_of, buf, i):
        for slot, m in enumerate(group_of):
            norm = jnp.sum(all_rows(functools.partial(scale_group, m), zeros), axis=0, keepdims=True) * inv_n[m] * inv_n[m]
            norm = jnp.sum(norm, axis=1, keepdims=True)
            w_sq = jnp.sum(jnp.sum(sq_sum[m], axis=0, keepdims=True), axis=1, keepdims=True)
            buf[me, slot] = jnp.where(lane < 32, norm, jnp.where(lane < 64, w_sq, row_mean[m]))
        for peer in peers:
            send(buf, me, send_s.at[i], recv_s.at[i], peer)

    def step_factor(buf, slot):
        got = buf[:, slot]
        s_full = jnp.sum(jnp.where(lane == 64, jnp.sum(got, axis=0), 0.0), axis=1, keepdims=True) / n_dev
        own = jnp.sum(jnp.where(lane == 64, buf[me, slot], 0.0), axis=1, keepdims=True)
        ratio = s_full[None] / pltpu.roll(got, 64, 2)
        acc = jnp.sum(got * jnp.where(lane[None] < 32, ratio, 1.0), axis=0)
        upd_sq = jnp.sum(jnp.where(lane == 0, acc, 0.0), axis=1, keepdims=True)
        w_sq = jnp.sum(jnp.where(lane == 32, acc, 0.0), axis=1, keepdims=True)
        upd_rms = jnp.sqrt(upd_sq / n_total)
        w_rms = jnp.sqrt(w_sq / n_total)
        size = hyper[1] * jnp.maximum(EPS_TWO, w_rms) / jnp.maximum(1.0, upd_rms / hyper[2])
        return size * jnp.sqrt(s_full / own)

    def update(group_of, buf, i):
        wait_bytes(buf.at[pl.ds(0, n_dev - 1)], recv_s.at[i])
        factors = [step_factor(buf, slot) * inv_n[m] for slot, m in enumerate(group_of)]
        for m, k in zip(group_of, factors):
            w_ref = weights(m)
            k = jnp.broadcast_to(k, (8, narrow))
            k = jnp.concatenate([k] * (group // 8), axis=0)

            def apply(at, r, carry, m=m, w_ref=w_ref, k=k):
                rows = slice(r, r + group)
                w = at(w_ref)
                w[rows, :] = w[rows, :] - k * at(upd.at[m])[rows, :]
                return carry
            all_rows(apply, 0)

    last = n_mat - 1
    for m in range(n_mat):
        total = zero
        copies = loads(m)
        blocks = order
        if m == 0:
            for copy in copies[:2]:
                copy.wait()
            for copy in loads(1):
                copy.start()
            total = products(m, split(0, 208, 224), total)
            blocks, copies = order[1:-1] + split(order[-1][0], 208, 208), copies[2:]
        for copy in copies:
            copy.wait()
        if 1 <= m < last:
            for copy in loads(m + 1):
                copy.start()
        w_copies[m].start()
        if m:
            w_copies[m - 1].wait()
        if m >= 2:
            wait_moments(m - 2)
            second_moments(m - 2)
        total = products(m, blocks, total)
        if m == 0:
            pl.semaphore_wait(barrier, n_dev - 1)
        send_moments(m, total)

    early, late = list(range(last)), [last]
    wait_moments(last - 1)
    second_moments(last - 1)
    w_copies[last].wait()
    for m in range(n_mat):
        sq_sum[m] = all_rows(functools.partial(square_group, m), zeros)
    send_scalars(early, rx_a, 0)
    wait_moments(last)
    second_moments(last)
    send_scalars(late, rx_b, 1)
    update(early, rx_a, 0)
    for m in range(n_mat):
        wait_bytes(rx_n.at[m, pl.ds(0, n_col - 1)], send_n.at[m])
        wait_bytes(rx_w.at[m, pl.ds(0, n_row - 1)], send_w.at[m])
    wait_bytes(rx_a.at[pl.ds(0, n_dev - 1)], send_s.at[0])
    wait_bytes(rx_b.at[pl.ds(0, n_dev - 1)], send_s.at[1])
    update(late, rx_b, 1)


def write_kernel(*refs):
    count = (len(refs) - 1) // 2
    srcs, dsts, sem = refs[:count], refs[count:2 * count], refs[-1]
    copies = []
    for src, dst in zip(srcs, dsts):
        if len(src.shape) == 2:
            pieces = [(src, dst)]
        else:
            rows = src.shape[1] // 2
            pieces = [(src.at[i, pl.ds(r, rows)], dst.at[i, pl.ds(r, rows)])
                      for i in range(src.shape[0]) for r in (0, rows)]
        for src_piece, dst_piece in pieces:
            copies.append(pltpu.make_async_copy(src_piece, dst_piece, sem.at[len(copies)]))
    for copy in copies:
        copy.start()
    for copy in copies:
        copy.wait()


def solution(mesh):
    n_col = mesh.shape['col']
    n_row = mesh.shape['row']
    tile_in = P(None, 'row', 'col')
    tile_out = P(None, 'col', 'row')
    lane_row = P(None, None, 'row')
    lane_col = P(None, None, 'col')
    vec_row = P(None, 'row')
    vec_col = P(None, 'col')

    def local_step(hyper_params, w_in, x_in, dy_in, row_in, col_in, w_out, x_out, dy_out, row_out, col_out):
        layers, narrow, wide = w_in.shape
        tokens = x_in.shape[1]
        n_mat = 2 * layers
        n_dev = n_col * n_row
        hbm = pl.BlockSpec(memory_space=pltpu.HBM)
        vmem = pl.BlockSpec(memory_space=pltpu.VMEM)
        smem = pl.BlockSpec(memory_space=pltpu.SMEM)
        dma = pltpu.SemaphoreType.DMA
        nr, wr = 8, 16
        swap = lambda v: jnp.swapaxes(v, 1, 2)
        sizes = (432, 416, 416, 416)
        shapes = [v.shape for v in (w_out, row_in, col_in, w_out, row_out, col_out)]
        results = pl.pallas_call(
            functools.partial(stats_kernel, n_col, n_row, sizes),
            out_shape=tuple(pltpu.VMEM(shape, F32) for shape in shapes),
            in_specs=[smem, hbm, hbm, hbm, vmem, vmem, hbm, hbm, hbm, vmem, vmem],
            out_specs=(vmem,) * 6,
            scratch_shapes=[
                pltpu.VMEM((n_mat, wide, narrow), F32),
                pltpu.VMEM((2, tokens, narrow), jnp.bfloat16),
                pltpu.VMEM((2, wide, tokens), jnp.bfloat16),
                pltpu.VMEM((wide, LANES), F32),
                pltpu.VMEM((n_mat, wide, LANES), F32),
                pltpu.VMEM((n_mat, 1, narrow), F32),
                pltpu.VMEM((n_mat, n_col, nr, LANES), F32),
                pltpu.VMEM((n_mat, n_row, wr, LANES), F32),
                pltpu.VMEM((n_dev, n_mat - 1, 1, LANES), F32),
                pltpu.VMEM((n_dev, 1, 1, LANES), F32),
                pltpu.VMEM((n_mat, nr, LANES), F32),
                pltpu.VMEM((n_mat, wr, LANES), F32),
                dma((2,)), dma((2, len(sizes))), dma((n_mat,)),
                dma((n_mat,)), dma((n_mat,)), dma((n_mat,)), dma((n_mat,)), dma((2,)), dma((2,)),
            ],
            compiler_params=pltpu.CompilerParams(collective_id=0, has_side_effects=True, vmem_limit_bytes=44 << 20),
            name="stats",
        )(hyper_params, swap(w_in), x_in, swap(dy_in), row_in, col_in, w_out, swap(x_out), dy_out, row_out, col_out)
        w_in_new, row_in_new, col_in_new, w_out_new, row_out_new, col_out_new = pl.pallas_call(
            write_kernel,
            out_shape=tuple(pltpu.HBM(shape, F32) for shape in shapes),
            in_specs=[vmem] * 6,
            out_specs=(hbm,) * 6,
            scratch_shapes=[dma((8 * layers + 4,))],
            compiler_params=pltpu.CompilerParams(vmem_limit_bytes=1 << 20),
            name="write",
        )(*(pltpu.with_memory_space_constraint(v, pltpu.VMEM) for v in results))
        return swap(w_in_new), row_in_new, col_in_new, w_out_new, row_out_new, col_out_new

    return jax.shard_map(local_step, mesh=mesh, in_specs=(P(), tile_in, lane_row, lane_col, vec_row, vec_col, tile_out, lane_col, lane_row, vec_col, vec_row), out_specs=(tile_in, vec_row, vec_col, tile_out, vec_col, vec_row), check_vma=False)
```

```python
import functools

import jax
import jax.numpy as jnp
from jax import lax
from jax.experimental import pallas as pl
from jax.experimental.pallas import tpu as pltpu
from jax.sharding import PartitionSpec as P

EPS_ONE = 1e-30
EPS_TWO = 1e-3
MESH = pl.DeviceIdType.MESH
F32 = jnp.float32
LANES = 128


def col_tiles(width):
    return [(start, min(LANES, width - start)) for start in range(0, width, LANES)]


def stats_kernel(n_col, n_row, sizes, main, hyper, w_in, x_in, dy_in, row_in, col_in, w_out, x_out, dy_out, row_out, col_out,
                 wv_in, row_in_new, col_in_new, wv_out, row_out_new, col_out_new,
                 upd, a_buf, b_buf, a_t, b_t, row_acc, w_col, inv_n, rx_n, rx_w, rx_a, rx_b, old_n, old_w,
                 a_sem, b_sem, w_sem, send_n, recv_n, send_w, recv_w, send_s, recv_s):
    n_mat, wide, narrow = upd.shape
    layers = n_mat // 2
    full_narrow, full_wide = narrow * n_row, wide * n_col
    n_total = float(full_narrow * full_wide)
    my_c, my_r = lax.axis_index("col"), lax.axis_index("row")
    n_dev = n_col * n_row
    me = my_c * n_row + my_r
    tiles = col_tiles(wide)
    nt = col_tiles(narrow)

    def split(start, *lengths):
        return [(start + sum(lengths[:i]), w) for i, w in enumerate(lengths)]

    order = split(0, *sizes)

    def loads(m):
        slot, layer = m % 2, m % layers
        a_src, b_src = (x_in, dy_in) if m < layers else (dy_out, x_out)
        return ([pltpu.make_async_copy(a_src.at[layer], a_buf.at[slot], a_sem.at[slot])]
                + [pltpu.make_async_copy(b_src.at[layer, pl.ds(s, w)], b_buf.at[slot, pl.ds(s, w)], b_sem.at[slot, i])
                   for i, (s, w) in enumerate(order)])

    for copy in loads(0):
        copy.start()
    barrier = pltpu.get_barrier_semaphore()
    peers_c = [lax.rem(my_c + d, n_col) for d in range(n_col)]
    peers_r = [lax.rem(my_r + d, n_row) for d in range(n_row)]
    peers = [(c, r) for i, c in enumerate(peers_c) for j, r in enumerate(peers_r) if i or j]
    for peer in peers:
        pl.semaphore_signal(barrier, inc=1, device_id=peer, device_id_type=MESH)

    old_n[...] = jnp.zeros_like(old_n)
    old_w[...] = jnp.zeros_like(old_w)
    for m in range(n_mat):
        rx_n[m, my_c] = jnp.zeros(rx_n.shape[2:], F32)
        rx_w[m, my_r] = jnp.zeros(rx_w.shape[2:], F32)
    for layer in range(layers):
        for m, src_n, src_w in ((layer, row_in, col_in), (layers + layer, col_out, row_out)):
            for j, (s, w) in enumerate(nt):
                old_n[m, j:j + 1, :w] = src_n[layer:layer + 1, s:s + w]
            for j, (s, w) in enumerate(tiles):
                old_w[m, j:j + 1, :w] = src_w[layer:layer + 1, s:s + w]

    w_copies = ([pltpu.make_async_copy(w_in.at[i], wv_in.at[i], w_sem.at[i]) for i in range(layers)]
                + [pltpu.make_async_copy(w_out.at[i], wv_out.at[i], w_sem.at[layers + i]) for i in range(layers)])

    def weights(m):
        return wv_in.at[m % layers] if m < layers else wv_out.at[m % layers]

    def send(buf, index, send_sem, recv_sem, peer):
        pltpu.make_async_remote_copy(src_ref=buf.at[index], dst_ref=buf.at[index], send_sem=send_sem, recv_sem=recv_sem,
                                     device_id=peer, device_id_type=MESH).start()

    def wait_bytes(ref, sem):
        pltpu.make_async_copy(ref, ref, sem).wait()

    lane = lax.broadcasted_iota(jnp.int32, (1, LANES), 1)
    zeros = jnp.zeros((16, narrow), F32)
    sq_sum = {}
    row_mean = {}

    group, stretch = 16, 336

    def scale_group(m, at, r, acc):
        rows = slice(r, r + group)
        g = at(upd.at[m])
        u = g[rows, :] * jnp.concatenate([at(w_col.at[m])[rows, :]] * len(nt), axis=1)
        g[rows, :] = u
        return acc + u * u

    def square_group(m, at, r, acc):
        v = at(weights(m))[r:r + group, :]
        return acc + v * v

    def all_rows(fn, init):
        def body(i, carry):
            at = lambda ref: ref.at[pl.ds(pl.multiple_of(i * stretch, stretch), stretch)]
            for r in range(0, stretch, group):
                carry = fn(at, r, carry)
            return carry
        return lax.fori_loop(0, wide // stretch, body, init)

    def products(m, blocks, total, first, square=None):
        slot = m % 2
        if first:
            a_t[...] = a_buf[slot, :, main:].T
        for i, (s, w) in enumerate(blocks):
            block = b_buf.at[slot, pl.ds(s, w)]
            b_t[i % 2, :, :w] = block[...].T
            left = jnp.dot(block[...], a_buf[slot, :, :main], preferred_element_type=F32)
            right = jnp.dot(a_t[...], b_t[i % 2, :, :w], preferred_element_type=F32).T
            upd[m, s:s + w, :main] = left
            upd[m, s:s + w, main:] = right
            q = left * left
            p = right * right
            total = total + jnp.concatenate([jnp.sum(v.reshape(w // 8, 8, v.shape[1]), axis=0) for v in (q, p)], axis=1)
            for t, tw in col_tiles(main):
                p = p + q[:, t:t + tw]
            row_acc[s:s + w, :] = p
            if square is not None:
                acc = sq_sum.get(square, zeros)
                for r in range(s, s + w, group):
                    acc = square_group(square, lambda ref: ref, r, acc)
                sq_sum[square] = acc
            for t, tw in tiles:
                if s < t + tw <= s + w:
                    block = row_acc[t:t + tw, :].T
                    j = t // LANES
                    rx_w[m, my_r, j:j + 1, :tw] = jnp.sum(block, axis=0, keepdims=True)
        return total

    def send_moments(m, total):
        sums = jnp.sum(total, axis=0, keepdims=True)
        for j, (t, tw) in enumerate(nt):
            rx_n[m, my_c, j:j + 1, :] = sums[:, t:t + tw]
        for c in peers_c[1:]:
            send(rx_n.at[m], my_c, send_n.at[m], recv_n.at[m], (c, my_r))
        for r in peers_r[1:]:
            send(rx_w.at[m], my_r, send_w.at[m], recv_w.at[m], (my_c, r))

    def wait_moments(m):
        wait_bytes(rx_n.at[m, pl.ds(0, n_col - 1)], recv_n.at[m])
        wait_bytes(rx_w.at[m, pl.ds(0, n_row - 1)], recv_w.at[m])

    def second_moments(m):
        beta = hyper[0]
        layer = m % layers
        sum_n = rx_n[m, 0]
        for src in range(1, n_col):
            sum_n = sum_n + rx_n[m, src]
        sum_w = rx_w[m, 0]
        for src in range(1, n_row):
            sum_w = sum_w + rx_w[m, src]
        new_n = beta * old_n[m] + (1.0 - beta) * (sum_n / full_wide + EPS_ONE)
        new_w = beta * old_w[m] + (1.0 - beta) * (sum_w / full_narrow + EPS_ONE)
        dst_n, dst_w = (row_in_new, col_in_new) if m < layers else (col_out_new, row_out_new)
        for j, (t, tw) in enumerate(nt):
            dst_n[layer:layer + 1, t:t + tw] = new_n[j:j + 1, :tw]
        for j, (t, tw) in enumerate(tiles):
            dst_w[layer:layer + 1, t:t + tw] = new_w[j:j + 1, :tw]
        v, length = (new_n, narrow) if m < layers else (new_w, wide)
        index = lax.broadcasted_iota(jnp.int32, v.shape, 0) * LANES + lax.broadcasted_iota(jnp.int32, v.shape, 1)
        mean = jnp.sum(jnp.sum(jnp.where(index < length, v, 0.0), axis=0, keepdims=True), axis=1, keepdims=True) / length
        row_mean[m] = mean
        root = jnp.sqrt(mean)
        scaled = lax.rsqrt(new_n) * root
        for j, (t, tw) in enumerate(nt):
            inv_n[m, :, t:t + tw] = scaled[j:j + 1, :]
        inv_w = lax.rsqrt(new_w)
        for j, (t, tw) in enumerate(tiles):
            w_col[m, t:t + tw, :] = jnp.broadcast_to(inv_w[j:j + 1, :tw], (LANES, tw)).T

    def send_scalars(group_of, buf, i):
        for slot, m in enumerate(group_of):
            norm = jnp.sum(all_rows(functools.partial(scale_group, m), zeros), axis=0, keepdims=True) * inv_n[m] * inv_n[m]
            norm = jnp.sum(norm, axis=1, keepdims=True)
            w_sq = jnp.sum(jnp.sum(sq_sum[m], axis=0, keepdims=True), axis=1, keepdims=True)
            buf[me, slot] = jnp.where(lane < 32, norm, jnp.where(lane < 64, w_sq, row_mean[m]))
        for peer in peers:
            send(buf, me, send_s.at[i], recv_s.at[i], peer)

    def step_factor(buf, slot):
        got = buf[:, slot]
        s_full = jnp.sum(jnp.where(lane == 64, jnp.sum(got, axis=0), 0.0), axis=1, keepdims=True) / n_dev
        own = jnp.sum(jnp.where(lane == 64, buf[me, slot], 0.0), axis=1, keepdims=True)
        ratio = s_full[None] / pltpu.roll(got, 64, 2)
        acc = jnp.sum(got * jnp.where(lane[None] < 32, ratio, 1.0), axis=0)
        upd_sq = jnp.sum(jnp.where(lane == 0, acc, 0.0), axis=1, keepdims=True)
        w_sq = jnp.sum(jnp.where(lane == 32, acc, 0.0), axis=1, keepdims=True)
        upd_rms = jnp.sqrt(upd_sq / n_total)
        w_rms = jnp.sqrt(w_sq / n_total)
        size = hyper[1] * jnp.maximum(EPS_TWO, w_rms) / jnp.maximum(1.0, upd_rms / hyper[2])
        return size * jnp.sqrt(s_full / own)

    def update(group_of, buf, i):
        wait_bytes(buf.at[pl.ds(0, n_dev - 1)], recv_s.at[i])
        factors = [step_factor(buf, slot) * inv_n[m] for slot, m in enumerate(group_of)]
        for m, k in zip(group_of, factors):
            w_ref = weights(m)
            k = jnp.broadcast_to(k, (8, narrow))
            k = jnp.concatenate([k] * (group // 8), axis=0)

            def apply(at, r, carry, m=m, w_ref=w_ref, k=k):
                rows = slice(r, r + group)
                w = at(w_ref)
                w[rows, :] = w[rows, :] - k * at(upd.at[m])[rows, :]
                return carry
            all_rows(apply, 0)

    last = n_mat - 1
    for m in range(n_mat):
        total = jnp.zeros((8, narrow), F32)
        copies = loads(m)
        blocks = order
        if m == 0:
            for copy in copies[:2]:
                copy.wait()
            for copy in loads(1):
                copy.start()
            total = products(m, order[:1], total, True)
            blocks, copies = order[1:], copies[2:]
        for copy in copies:
            copy.wait()
        if 1 <= m < last:
            for copy in loads(m + 1):
                copy.start()
        w_copies[m].start()
        if m:
            w_copies[m - 1].wait()
        if m >= 2:
            wait_moments(m - 2)
            second_moments(m - 2)
        total = products(m, blocks, total, m > 0)
        if m == 0:
            pl.semaphore_wait(barrier, n_dev - 1)
        send_moments(m, total)

    early, late = list(range(last)), [last]
    wait_moments(last - 1)
    second_moments(last - 1)
    w_copies[last].wait()
    for m in range(n_mat):
        sq_sum[m] = all_rows(functools.partial(square_group, m), zeros)
    send_scalars(early, rx_a, 0)
    wait_moments(last)
    second_moments(last)
    send_scalars(late, rx_b, 1)
    update(early, rx_a, 0)
    for m in range(n_mat):
        wait_bytes(rx_n.at[m, pl.ds(0, n_col - 1)], send_n.at[m])
        wait_bytes(rx_w.at[m, pl.ds(0, n_row - 1)], send_w.at[m])
    wait_bytes(rx_a.at[pl.ds(0, n_dev - 1)], send_s.at[0])
    wait_bytes(rx_b.at[pl.ds(0, n_dev - 1)], send_s.at[1])
    update(late, rx_b, 1)


def write_kernel(*refs):
    count = (len(refs) - 1) // 2
    srcs, dsts, sem = refs[:count], refs[count:2 * count], refs[-1]
    copies = []
    for src, dst in zip(srcs, dsts):
        if len(src.shape) == 2:
            pieces = [(src, dst)]
        else:
            rows = src.shape[1] // 2
            pieces = [(src.at[i, pl.ds(r, rows)], dst.at[i, pl.ds(r, rows)])
                      for i in range(src.shape[0]) for r in (0, rows)]
        for src_piece, dst_piece in pieces:
            copies.append(pltpu.make_async_copy(src_piece, dst_piece, sem.at[len(copies)]))
    for copy in copies:
        copy.start()
    for copy in copies:
        copy.wait()


def solution(mesh):
    n_col = mesh.shape['col']
    n_row = mesh.shape['row']
    tile_in = P(None, 'row', 'col')
    tile_out = P(None, 'col', 'row')
    lane_row = P(None, None, 'row')
    lane_col = P(None, None, 'col')
    vec_row = P(None, 'row')
    vec_col = P(None, 'col')

    def local_step(hyper_params, w_in, x_in, dy_in, row_in, col_in, w_out, x_out, dy_out, row_out, col_out):
        layers, narrow, wide = w_in.shape
        tokens = x_in.shape[1]
        n_mat = 2 * layers
        n_dev = n_col * n_row
        hbm = pl.BlockSpec(memory_space=pltpu.HBM)
        vmem = pl.BlockSpec(memory_space=pltpu.VMEM)
        smem = pl.BlockSpec(memory_space=pltpu.SMEM)
        dma = pltpu.SemaphoreType.DMA
        nr, wr = 8, 16
        swap = lambda v: jnp.swapaxes(v, 1, 2)
        sizes = (512, 512, 512, 144)
        main = narrow - LANES
        shapes = [v.shape for v in (w_out, row_in, col_in, w_out, row_out, col_out)]
        results = pl.pallas_call(
            functools.partial(stats_kernel, n_col, n_row, sizes, main),
            out_shape=tuple(pltpu.VMEM(shape, F32) for shape in shapes),
            in_specs=[smem, hbm, hbm, hbm, vmem, vmem, hbm, hbm, hbm, vmem, vmem],
            out_specs=(vmem,) * 6,
            scratch_shapes=[
                pltpu.VMEM((n_mat, wide, narrow), F32),
                pltpu.VMEM((2, tokens, narrow), jnp.bfloat16),
                pltpu.VMEM((2, wide, tokens), jnp.bfloat16),
                pltpu.VMEM((narrow - main, tokens), jnp.bfloat16),
                pltpu.VMEM((2, tokens, max(sizes)), jnp.bfloat16),
                pltpu.VMEM((wide, LANES), F32),
                pltpu.VMEM((n_mat, wide, LANES), F32),
                pltpu.VMEM((n_mat, 1, narrow), F32),
                pltpu.VMEM((n_mat, n_col, nr, LANES), F32),
                pltpu.VMEM((n_mat, n_row, wr, LANES), F32),
                pltpu.VMEM((n_dev, n_mat - 1, 1, LANES), F32),
                pltpu.VMEM((n_dev, 1, 1, LANES), F32),
                pltpu.VMEM((n_mat, nr, LANES), F32),
                pltpu.VMEM((n_mat, wr, LANES), F32),
                dma((2,)), dma((2, len(sizes))), dma((n_mat,)),
                dma((n_mat,)), dma((n_mat,)), dma((n_mat,)), dma((n_mat,)), dma((2,)), dma((2,)),
            ],
            compiler_params=pltpu.CompilerParams(collective_id=0, has_side_effects=True, vmem_limit_bytes=46 << 20),
            name="stats",
        )(hyper_params, swap(w_in), x_in, swap(dy_in), row_in, col_in, w_out, swap(x_out), dy_out, row_out, col_out)
        w_in_new, row_in_new, col_in_new, w_out_new, row_out_new, col_out_new = pl.pallas_call(
            write_kernel,
            out_shape=tuple(pltpu.HBM(shape, F32) for shape in shapes),
            in_specs=[vmem] * 6,
            out_specs=(hbm,) * 6,
            scratch_shapes=[dma((8 * layers + 4,))],
            compiler_params=pltpu.CompilerParams(vmem_limit_bytes=1 << 20),
            name="write",
        )(*(pltpu.with_memory_space_constraint(v, pltpu.VMEM) for v in results))
        return swap(w_in_new), row_in_new, col_in_new, w_out_new, row_out_new, col_out_new

    return jax.shard_map(local_step, mesh=mesh, in_specs=(P(), tile_in, lane_row, lane_col, vec_row, vec_col, tile_out, lane_col, lane_row, vec_col, vec_row), out_specs=(tile_in, vec_row, vec_col, tile_out, vec_col, vec_row), check_vma=False)
```

```python
import functools

import jax
import jax.numpy as jnp
from jax import lax
from jax.experimental import pallas as pl
from jax.experimental.pallas import tpu as pltpu
from jax.sharding import PartitionSpec as P

EPS_ONE = 1e-30
EPS_TWO = 1e-3
MESH = pl.DeviceIdType.MESH
F32 = jnp.float32
LANES = 128


def col_tiles(width):
    return [(start, min(LANES, width - start)) for start in range(0, width, LANES)]


def stats_kernel(n_col, n_row, sizes, main, hyper, w_in, x_in, dy_in, row_in, col_in, w_out, x_out, dy_out, row_out, col_out,
                 wv_in, row_in_new, col_in_new, wv_out, row_out_new, col_out_new, last_grad, last_factor,
                 upd, a_buf, b_buf, a_t, b_t, row_acc, w_col, inv_n, rx_n, rx_w, rx_a, rx_b, old_n, old_w,
                 a_sem, b_sem, w_sem, send_n, recv_n, send_w, recv_w, send_s, recv_s):
    layers, wide, narrow = wv_in.shape
    n_mat = 2 * layers
    last = n_mat - 1
    full_narrow, full_wide = narrow * n_row, wide * n_col
    n_total = float(full_narrow * full_wide)
    my_c, my_r = lax.axis_index("col"), lax.axis_index("row")
    n_dev = n_col * n_row
    me = my_c * n_row + my_r
    tiles = col_tiles(wide)
    nt = col_tiles(narrow)

    def split(start, *lengths):
        return [(start + sum(lengths[:i]), w) for i, w in enumerate(lengths)]

    order = split(0, *sizes)

    def loads(m):
        slot, layer = m % 2, m % layers
        a_src, b_src = (x_in, dy_in) if m < layers else (dy_out, x_out)
        return ([pltpu.make_async_copy(a_src.at[layer], a_buf.at[slot], a_sem.at[slot])]
                + [pltpu.make_async_copy(b_src.at[layer, pl.ds(s, w)], b_buf.at[slot, pl.ds(s, w)], b_sem.at[slot, i])
                   for i, (s, w) in enumerate(order)])

    for copy in loads(0):
        copy.start()
    barrier = pltpu.get_barrier_semaphore()
    flip = lambda v: v + 1 - 2 * lax.rem(v, 2)
    peers_c = [(n_col - 1 - my_c, 2), (lax.rem(my_c + 2, n_col), 1), (flip(my_c), 1), (my_c, 0)]
    peers_r = [(n_row - 1 - my_r, 1), (lax.rem(my_r + 2, n_row), 1), (flip(my_r), 0), (my_r, 0)]
    peers = sorted(((hops_c + hops_r, i, j) for i, (_, hops_c) in enumerate(peers_c) for j, (_, hops_r) in enumerate(peers_r)
                    if (i, j) != (3, 3)), reverse=True)
    peers = [(peers_c[i][0], peers_r[j][0]) for _, i, j in peers]
    for peer in peers:
        pl.semaphore_signal(barrier, inc=1, device_id=peer, device_id_type=MESH)

    old_n[...] = jnp.zeros_like(old_n)
    old_w[...] = jnp.zeros_like(old_w)
    for m in range(n_mat):
        rx_n[m, my_c] = jnp.zeros(rx_n.shape[2:], F32)
        rx_w[m, my_r] = jnp.zeros(rx_w.shape[2:], F32)
    for layer in range(layers):
        for m, src_n, src_w in ((layer, row_in, col_in), (layers + layer, col_out, row_out)):
            for j, (s, w) in enumerate(nt):
                old_n[m, j:j + 1, :w] = src_n[layer:layer + 1, s:s + w]
            for j, (s, w) in enumerate(tiles):
                old_w[m, j:j + 1, :w] = src_w[layer:layer + 1, s:s + w]

    w_copies = ([pltpu.make_async_copy(w_in.at[i], wv_in.at[i], w_sem.at[i]) for i in range(layers)]
                + [pltpu.make_async_copy(w_out.at[i], wv_out.at[i], w_sem.at[layers + i]) for i in range(layers)])

    def grad(m):
        return upd.at[m] if m < last else last_grad

    def weights(m):
        return wv_in.at[m % layers] if m < layers else wv_out.at[m % layers]

    def send(buf, index, send_sem, recv_sem, peer):
        pltpu.make_async_remote_copy(src_ref=buf.at[index], dst_ref=buf.at[index], send_sem=send_sem, recv_sem=recv_sem,
                                     device_id=peer, device_id_type=MESH).start()

    def wait_bytes(ref, sem):
        pltpu.make_async_copy(ref, ref, sem).wait()

    zeros = jnp.zeros((16, narrow), F32)
    sq_sum = {}
    row_mean = {}

    group, stretch = 16, 336

    def scale_group(m, at, r, acc):
        rows = slice(r, r + group)
        g = at(grad(m))
        u = g[rows, :] * jnp.concatenate([at(w_col.at[m])[rows, :]] * len(nt), axis=1)
        g[rows, :] = u
        return acc + u * u

    def square_group(m, at, r, acc):
        v = at(weights(m))[r:r + group, :]
        return acc + v * v

    def all_rows(fn, init):
        def body(i, carry):
            at = lambda ref: ref.at[pl.ds(pl.multiple_of(i * stretch, stretch), stretch)]
            for r in range(0, stretch, group):
                carry = fn(at, r, carry)
            return carry
        return lax.fori_loop(0, wide // stretch, body, init)

    def products(m, blocks, total, first):
        slot = m % 2
        if first:
            a_t[...] = a_buf[slot, :, main:].T
        for i, (s, w) in enumerate(blocks):
            block = b_buf.at[slot, pl.ds(s, w)]
            b_t[i % 2, :, :w] = block[...].T
            left = jnp.dot(block[...], a_buf[slot, :, :main], preferred_element_type=F32)
            right = jnp.dot(a_t[...], b_t[i % 2, :, :w], preferred_element_type=F32).T
            grad(m)[s:s + w, :main] = left
            grad(m)[s:s + w, main:] = right
            q = left * left
            p = right * right
            total = total + jnp.concatenate([jnp.sum(v.reshape(w // 8, 8, v.shape[1]), axis=0) for v in (q, p)], axis=1)
            for t, tw in col_tiles(main):
                p = p + q[:, t:t + tw]
            row_acc[s:s + w, :] = p
            for t, tw in tiles:
                if s < t + tw <= s + w:
                    block = row_acc[t:t + tw, :].T
                    j = t // LANES
                    rx_w[m, my_r, j:j + 1, :tw] = jnp.sum(block, axis=0, keepdims=True)
        return total

    def send_moments(m, total):
        sums = jnp.sum(total, axis=0, keepdims=True)
        for j, (t, tw) in enumerate(nt):
            rx_n[m, my_c, j:j + 1, :] = sums[:, t:t + tw]
        for c, _ in peers_c[:-1]:
            send(rx_n.at[m], my_c, send_n.at[m], recv_n.at[m], (c, my_r))
        for r, _ in peers_r[:-1]:
            send(rx_w.at[m], my_r, send_w.at[m], recv_w.at[m], (my_c, r))

    def wait_moments(m):
        wait_bytes(rx_n.at[m, pl.ds(0, n_col - 1)], recv_n.at[m])
        wait_bytes(rx_w.at[m, pl.ds(0, n_row - 1)], recv_w.at[m])

    def second_moments(m):
        beta = hyper[0]
        layer = m % layers
        sum_n = rx_n[m, 0]
        for src in range(1, n_col):
            sum_n = sum_n + rx_n[m, src]
        sum_w = rx_w[m, 0]
        for src in range(1, n_row):
            sum_w = sum_w + rx_w[m, src]
        new_n = beta * old_n[m] + (1.0 - beta) * (sum_n / full_wide + EPS_ONE)
        new_w = beta * old_w[m] + (1.0 - beta) * (sum_w / full_narrow + EPS_ONE)
        dst_n, dst_w = (row_in_new, col_in_new) if m < layers else (col_out_new, row_out_new)
        for j, (t, tw) in enumerate(nt):
            dst_n[layer:layer + 1, t:t + tw] = new_n[j:j + 1, :tw]
        for j, (t, tw) in enumerate(tiles):
            dst_w[layer:layer + 1, t:t + tw] = new_w[j:j + 1, :tw]
        v, length = (new_n, narrow) if m < layers else (new_w, wide)
        index = lax.broadcasted_iota(jnp.int32, v.shape, 0) * LANES + lax.broadcasted_iota(jnp.int32, v.shape, 1)
        mean = jnp.sum(jnp.sum(jnp.where(index < length, v, 0.0), axis=0, keepdims=True), axis=1, keepdims=True) / length
        row_mean[m] = mean
        root = jnp.sqrt(mean)
        scaled = lax.rsqrt(new_n) * root
        for j, (t, tw) in enumerate(nt):
            inv_n[m, :, t:t + tw] = scaled[j:j + 1, :]
        inv_w = lax.rsqrt(new_w)
        for j, (t, tw) in enumerate(tiles):
            w_col[m, t:t + tw, :] = jnp.broadcast_to(inv_w[j:j + 1, :tw], (LANES, tw)).T

    def send_scalars(group_of, buf, i):
        for slot, m in enumerate(group_of):
            norm = jnp.sum(all_rows(functools.partial(scale_group, m), zeros), axis=0, keepdims=True) * inv_n[m] * inv_n[m]
            norm = jnp.sum(norm, axis=1, keepdims=True)
            w_sq = jnp.sum(jnp.sum(sq_sum[m], axis=0, keepdims=True), axis=1, keepdims=True)
            for row, v in enumerate((norm, w_sq, row_mean[m])):
                buf[me, 3 * slot + row] = jnp.broadcast_to(v, (1, LANES))
        for peer in peers:
            send(buf, me, send_s.at[i], recv_s.at[i], peer)

    def step_factor(buf, slot):
        norms, w_sqs, means = (buf[:, 3 * slot + row] for row in range(3))
        s_full = jnp.sum(means, axis=0) / n_dev
        own = buf[me, 3 * slot + 2]
        upd_sq = jnp.sum(norms * (s_full[None] / means), axis=0)
        w_sq = jnp.sum(w_sqs, axis=0)
        upd_rms = jnp.sqrt(upd_sq / n_total)
        w_rms = jnp.sqrt(w_sq / n_total)
        size = hyper[1] * jnp.maximum(EPS_TWO, w_rms) / jnp.maximum(1.0, upd_rms / hyper[2])
        return size * jnp.sqrt(s_full / own)

    def update(group_of, buf, i):
        wait_bytes(buf.at[pl.ds(0, n_dev - 1)], recv_s.at[i])
        factors = [jnp.concatenate([step_factor(buf, slot)] * len(nt), axis=1) * inv_n[m] for slot, m in enumerate(group_of)]
        for m, k in zip(group_of, factors):
            if m == last:
                last_factor[...] = k
                return
            w_ref = weights(m)
            k = jnp.broadcast_to(k, (8, narrow))
            k = jnp.concatenate([k] * (group // 8), axis=0)

            def apply(at, r, carry, m=m, w_ref=w_ref, k=k):
                rows = slice(r, r + group)
                w = at(w_ref)
                w[rows, :] = w[rows, :] - k * at(grad(m))[rows, :]
                return carry
            all_rows(apply, 0)

    for m in range(n_mat):
        total = jnp.zeros((8, narrow), F32)
        copies = loads(m)
        blocks = order
        if m == 0:
            for copy in copies[:2]:
                copy.wait()
            for copy in loads(1):
                copy.start()
            total = products(m, order[:1], total, True)
            blocks, copies = order[1:], copies[2:]
        for copy in copies:
            copy.wait()
        if 1 <= m < last:
            for copy in loads(m + 1):
                copy.start()
        w_copies[m].start()
        if m >= 2:
            wait_moments(m - 2)
            second_moments(m - 2)
        total = products(m, blocks, total, m > 0)
        if m == 0:
            pl.semaphore_wait(barrier, n_dev - 1)
        send_moments(m, total)

    early, late = list(range(last)), [last]
    wait_moments(last - 1)
    second_moments(last - 1)
    for m in range(n_mat):
        w_copies[m].wait()
        sq_sum[m] = all_rows(functools.partial(square_group, m), zeros)
    send_scalars(early, rx_a, 0)
    wait_moments(last)
    second_moments(last)
    send_scalars(late, rx_b, 1)
    update(early, rx_a, 0)
    for m in range(n_mat):
        wait_bytes(rx_n.at[m, pl.ds(0, n_col - 1)], send_n.at[m])
        wait_bytes(rx_w.at[m, pl.ds(0, n_row - 1)], send_w.at[m])
    wait_bytes(rx_a.at[pl.ds(0, n_dev - 1)], send_s.at[0])
    wait_bytes(rx_b.at[pl.ds(0, n_dev - 1)], send_s.at[1])
    update(late, rx_b, 1)


def write_kernel(*refs):
    count = (len(refs) - 4) // 2
    srcs, (grad, factor), dsts, (stage, sem) = refs[:count], refs[count:count + 2], refs[count + 2:-2], refs[-2:]
    layers, wide, _ = srcs[3].shape
    copies = []

    def copy(src, dst):
        copies.append(pltpu.make_async_copy(src, dst, sem.at[len(copies)]))
        copies[-1].start()

    rows = wide // 2
    for src, dst in ((srcs[0], dsts[0]), (srcs[3], dsts[3])):
        for i in range(layers):
            if src is not srcs[3] or i < layers - 1:
                for r in (0, rows):
                    copy(src.at[i, pl.ds(r, rows)], dst.at[i, pl.ds(r, rows)])
    for i in (1, 2, 4, 5):
        copy(srcs[i], dsts[i])
    step = wide // 5
    k = factor[...]
    for r in range(0, wide, step):
        for t in range(r, r + step, 16):
            stage[t:t + 16, :] = srcs[3][layers - 1, t:t + 16, :] - k * grad[t:t + 16, :]
        copy(stage.at[pl.ds(r, step)], dsts[3].at[layers - 1, pl.ds(r, step)])
    for item in copies:
        item.wait()


def solution(mesh):
    n_col = mesh.shape['col']
    n_row = mesh.shape['row']
    tile_in = P(None, 'row', 'col')
    tile_out = P(None, 'col', 'row')
    lane_row = P(None, None, 'row')
    lane_col = P(None, None, 'col')
    vec_row = P(None, 'row')
    vec_col = P(None, 'col')

    def local_step(hyper_params, w_in, x_in, dy_in, row_in, col_in, w_out, x_out, dy_out, row_out, col_out):
        layers, narrow, wide = w_in.shape
        tokens = x_in.shape[1]
        n_mat = 2 * layers
        n_dev = n_col * n_row
        hbm = pl.BlockSpec(memory_space=pltpu.HBM)
        vmem = pl.BlockSpec(memory_space=pltpu.VMEM)
        smem = pl.BlockSpec(memory_space=pltpu.SMEM)
        dma = pltpu.SemaphoreType.DMA
        nr, wr = 8, 16
        swap = lambda v: jnp.swapaxes(v, 1, 2)
        sizes = (512, 512, 512, 144)
        main = narrow - LANES
        shapes = [v.shape for v in (w_out, row_in, col_in, w_out, row_out, col_out)]
        results = pl.pallas_call(
            functools.partial(stats_kernel, n_col, n_row, sizes, main),
            out_shape=tuple(pltpu.VMEM(shape, F32) for shape in shapes + [w_out.shape[1:], (1, narrow)]),
            in_specs=[smem, hbm, hbm, hbm, vmem, vmem, hbm, hbm, hbm, vmem, vmem],
            out_specs=(vmem,) * 8,
            scratch_shapes=[
                pltpu.VMEM((n_mat - 1, wide, narrow), F32),
                pltpu.VMEM((2, tokens, narrow), jnp.bfloat16),
                pltpu.VMEM((2, wide, tokens), jnp.bfloat16),
                pltpu.VMEM((narrow - main, tokens), jnp.bfloat16),
                pltpu.VMEM((2, tokens, max(sizes)), jnp.bfloat16),
                pltpu.VMEM((wide, LANES), F32),
                pltpu.VMEM((n_mat, wide, LANES), F32),
                pltpu.VMEM((n_mat, 1, narrow), F32),
                pltpu.VMEM((n_mat, n_col, nr, LANES), F32),
                pltpu.VMEM((n_mat, n_row, wr, LANES), F32),
                pltpu.VMEM((n_dev, 3 * (n_mat - 1), 1, LANES), F32),
                pltpu.VMEM((n_dev, 3, 1, LANES), F32),
                pltpu.VMEM((n_mat, nr, LANES), F32),
                pltpu.VMEM((n_mat, wr, LANES), F32),
                dma((2,)), dma((2, len(sizes))), dma((n_mat,)),
                dma((n_mat,)), dma((n_mat,)), dma((n_mat,)), dma((n_mat,)), dma((2,)), dma((2,)),
            ],
            compiler_params=pltpu.CompilerParams(collective_id=0, has_side_effects=True, vmem_limit_bytes=42 << 20),
            name="stats",
        )(hyper_params, swap(w_in), x_in, swap(dy_in), row_in, col_in, w_out, swap(x_out), dy_out, row_out, col_out)
        w_in_new, row_in_new, col_in_new, w_out_new, row_out_new, col_out_new = pl.pallas_call(
            write_kernel,
            out_shape=tuple(pltpu.HBM(shape, F32) for shape in shapes),
            in_specs=[vmem] * 8,
            out_specs=(hbm,) * 6,
            scratch_shapes=[pltpu.VMEM(w_out.shape[1:], F32), dma((4 * layers + 7,))],
            compiler_params=pltpu.CompilerParams(vmem_limit_bytes=6 << 20),
            name="write",
        )(*(pltpu.with_memory_space_constraint(v, pltpu.VMEM) for v in results))
        return swap(w_in_new), row_in_new, col_in_new, w_out_new, row_out_new, col_out_new

    return jax.shard_map(local_step, mesh=mesh, in_specs=(P(), tile_in, lane_row, lane_col, vec_row, vec_col, tile_out, lane_col, lane_row, vec_col, vec_row), out_specs=(tile_in, vec_row, vec_col, tile_out, vec_col, vec_row), check_vma=False)
```

```python
import functools

import jax
import jax.numpy as jnp
from jax import lax
from jax.experimental import pallas as pl
from jax.experimental.pallas import tpu as pltpu
from jax.sharding import PartitionSpec as P

EPS_ONE = 1e-30
EPS_TWO = 1e-3
MESH = pl.DeviceIdType.MESH
F32 = jnp.float32
LANES = 128


def col_tiles(width):
    return [(start, min(LANES, width - start)) for start in range(0, width, LANES)]


def stats_kernel(n_col, n_row, sizes, main, hyper, w_in, x_in, dy_in, row_in, col_in, w_out, x_out, dy_out, row_out, col_out,
                 wv_in, row_in_new, col_in_new, wv_out, row_out_new, col_out_new, last_grad, last_factor,
                 upd, a_buf, b_buf, a_t, b_t, row_acc, w_col, inv_n, rx_n, rx_w, rx_a, rx_b, old_n, old_w,
                 a_sem, b_sem, w_sem, send_n, recv_n, send_w, recv_w, send_s, recv_s):
    layers, wide, narrow = wv_in.shape
    n_mat = 2 * layers
    last = n_mat - 1
    kept = n_mat - layers
    full_narrow, full_wide = narrow * n_row, wide * n_col
    n_total = float(full_narrow * full_wide)
    my_c, my_r = lax.axis_index("col"), lax.axis_index("row")
    n_dev = n_col * n_row
    me = my_c * n_row + my_r
    tiles = col_tiles(wide)
    nt = col_tiles(narrow)

    def split(start, *lengths):
        return [(start + sum(lengths[:i]), w) for i, w in enumerate(lengths)]

    order = split(0, *sizes)

    def loads(m):
        slot, layer = m % 2, m % layers
        a_src, b_src = (x_in, dy_in) if m < layers else (dy_out, x_out)
        return ([pltpu.make_async_copy(a_src.at[layer], a_buf.at[slot], a_sem.at[slot])]
                + [pltpu.make_async_copy(b_src.at[layer, pl.ds(s, w)], b_buf.at[slot, pl.ds(s, w)], b_sem.at[slot, i])
                   for i, (s, w) in enumerate(order)])

    for copy in loads(0):
        copy.start()
    barrier = pltpu.get_barrier_semaphore()
    flip = lambda v: v + 1 - 2 * lax.rem(v, 2)
    peers_c = [(n_col - 1 - my_c, 2), (lax.rem(my_c + 2, n_col), 1), (flip(my_c), 1), (my_c, 0)]
    peers_r = [(n_row - 1 - my_r, 1), (lax.rem(my_r + 2, n_row), 1), (flip(my_r), 0), (my_r, 0)]
    peers = sorted(((hops_c + hops_r, i, j) for i, (_, hops_c) in enumerate(peers_c) for j, (_, hops_r) in enumerate(peers_r)
                    if (i, j) != (3, 3)), reverse=True)
    peers = [(peers_c[i][0], peers_r[j][0]) for _, i, j in peers]
    for peer in peers:
        pl.semaphore_signal(barrier, inc=1, device_id=peer, device_id_type=MESH)

    old_n[...] = jnp.zeros_like(old_n)
    old_w[...] = jnp.zeros_like(old_w)
    for m in range(n_mat):
        rx_n[m, my_c] = jnp.zeros(rx_n.shape[2:], F32)
        rx_w[m, my_r] = jnp.zeros(rx_w.shape[2:], F32)
    for layer in range(layers):
        for m, src_n, src_w in ((layer, row_in, col_in), (layers + layer, col_out, row_out)):
            for j, (s, w) in enumerate(nt):
                old_n[m, j:j + 1, :w] = src_n[layer:layer + 1, s:s + w]
            for j, (s, w) in enumerate(tiles):
                old_w[m, j:j + 1, :w] = src_w[layer:layer + 1, s:s + w]

    w_copies = ([pltpu.make_async_copy(w_in.at[i], wv_in.at[i], w_sem.at[i]) for i in range(layers)]
                + [pltpu.make_async_copy(w_out.at[i], wv_out.at[i], w_sem.at[layers + i]) for i in range(layers)])

    def grad(m):
        return upd.at[m] if m < kept else last_grad.at[m - kept]

    def weights(m):
        return wv_in.at[m % layers] if m < layers else wv_out.at[m % layers]

    def send(buf, index, send_sem, recv_sem, peer):
        pltpu.make_async_remote_copy(src_ref=buf.at[index], dst_ref=buf.at[index], send_sem=send_sem, recv_sem=recv_sem,
                                     device_id=peer, device_id_type=MESH).start()

    def wait_bytes(ref, sem):
        pltpu.make_async_copy(ref, ref, sem).wait()

    zeros = jnp.zeros((16, narrow), F32)
    sq_sum = {}
    row_mean = {}

    group, stretch = 16, 336

    def scale_group(m, at, r, acc):
        rows = slice(r, r + group)
        g = at(grad(m))
        u = g[rows, :] * jnp.concatenate([at(w_col.at[m])[rows, :]] * len(nt), axis=1)
        g[rows, :] = u
        return acc + u * u

    def square_group(m, at, r, acc):
        v = at(weights(m))[r:r + group, :]
        return acc + v * v

    def both_group(m, at, r, accs):
        return scale_group(m, at, r, accs[0]), square_group(m, at, r, accs[1])

    def all_rows(fn, init):
        def body(i, carry):
            at = lambda ref: ref.at[pl.ds(pl.multiple_of(i * stretch, stretch), stretch)]
            for r in range(0, stretch, group):
                carry = fn(at, r, carry)
            return carry
        return lax.fori_loop(0, wide // stretch, body, init)

    def products(m, blocks, total, first):
        slot = m % 2
        if first:
            a_t[...] = a_buf[slot, :, main:].T
        for i, (s, w) in enumerate(blocks):
            block = b_buf.at[slot, pl.ds(s, w)]
            b_t[i % 2, :, :w] = block[...].T
            left = jnp.dot(block[...], a_buf[slot, :, :main], preferred_element_type=F32)
            right = jnp.dot(a_t[...], b_t[i % 2, :, :w], preferred_element_type=F32).T
            grad(m)[s:s + w, :main] = left
            grad(m)[s:s + w, main:] = right
            q = left * left
            p = right * right
            total = total + jnp.concatenate([jnp.sum(v.reshape(w // 8, 8, v.shape[1]), axis=0) for v in (q, p)], axis=1)
            for t, tw in col_tiles(main):
                p = p + q[:, t:t + tw]
            row_acc[s:s + w, :] = p
            for t, tw in tiles:
                if s < t + tw <= s + w:
                    block = row_acc[t:t + tw, :].T
                    j = t // LANES
                    rx_w[m, my_r, j:j + 1, :tw] = jnp.sum(block, axis=0, keepdims=True)
        return total

    def send_moments(m, total):
        sums = jnp.sum(total, axis=0, keepdims=True)
        for j, (t, tw) in enumerate(nt):
            rx_n[m, my_c, j:j + 1, :] = sums[:, t:t + tw]
        for c, _ in peers_c[:-1]:
            send(rx_n.at[m], my_c, send_n.at[m], recv_n.at[m], (c, my_r))
        for r, _ in peers_r[:-1]:
            send(rx_w.at[m], my_r, send_w.at[m], recv_w.at[m], (my_c, r))

    def wait_moments(m):
        wait_bytes(rx_n.at[m, pl.ds(0, n_col - 1)], recv_n.at[m])
        wait_bytes(rx_w.at[m, pl.ds(0, n_row - 1)], recv_w.at[m])

    def second_moments(m):
        beta = hyper[0]
        layer = m % layers
        sum_n = rx_n[m, 0]
        for src in range(1, n_col):
            sum_n = sum_n + rx_n[m, src]
        sum_w = rx_w[m, 0]
        for src in range(1, n_row):
            sum_w = sum_w + rx_w[m, src]
        new_n = beta * old_n[m] + (1.0 - beta) * (sum_n / full_wide + EPS_ONE)
        new_w = beta * old_w[m] + (1.0 - beta) * (sum_w / full_narrow + EPS_ONE)
        dst_n, dst_w = (row_in_new, col_in_new) if m < layers else (col_out_new, row_out_new)
        for j, (t, tw) in enumerate(nt):
            dst_n[layer:layer + 1, t:t + tw] = new_n[j:j + 1, :tw]
        for j, (t, tw) in enumerate(tiles):
            dst_w[layer:layer + 1, t:t + tw] = new_w[j:j + 1, :tw]
        v, length = (new_n, narrow) if m < layers else (new_w, wide)
        index = lax.broadcasted_iota(jnp.int32, v.shape, 0) * LANES + lax.broadcasted_iota(jnp.int32, v.shape, 1)
        mean = jnp.sum(jnp.sum(jnp.where(index < length, v, 0.0), axis=0, keepdims=True), axis=1, keepdims=True) / length
        row_mean[m] = mean
        root = jnp.sqrt(mean)
        scaled = lax.rsqrt(new_n) * root
        for j, (t, tw) in enumerate(nt):
            inv_n[m, :, t:t + tw] = scaled[j:j + 1, :]
        inv_w = lax.rsqrt(new_w)
        for j, (t, tw) in enumerate(tiles):
            w_col[m, t:t + tw, :] = jnp.broadcast_to(inv_w[j:j + 1, :tw], (LANES, tw)).T

    def send_scalars(group_of, buf, i):
        for slot, m in enumerate(group_of):
            if m in sq_sum:
                norm = all_rows(functools.partial(scale_group, m), zeros)
            else:
                norm, sq_sum[m] = all_rows(functools.partial(both_group, m), (zeros, zeros))
            norm = jnp.sum(norm, axis=0, keepdims=True) * inv_n[m] * inv_n[m]
            norm = jnp.sum(norm, axis=1, keepdims=True)
            w_sq = jnp.sum(jnp.sum(sq_sum[m], axis=0, keepdims=True), axis=1, keepdims=True)
            for row, v in enumerate((norm, w_sq, row_mean[m])):
                buf[me, 3 * slot + row] = jnp.broadcast_to(v, (1, LANES))
        for peer in peers:
            send(buf, me, send_s.at[i], recv_s.at[i], peer)

    def step_factor(buf, slot):
        norms, w_sqs, means = (buf[:, 3 * slot + row] for row in range(3))
        s_full = jnp.sum(means, axis=0) / n_dev
        own = buf[me, 3 * slot + 2]
        upd_sq = jnp.sum(norms * (s_full[None] / means), axis=0)
        w_sq = jnp.sum(w_sqs, axis=0)
        upd_rms = jnp.sqrt(upd_sq / n_total)
        w_rms = jnp.sqrt(w_sq / n_total)
        size = hyper[1] * jnp.maximum(EPS_TWO, w_rms) / jnp.maximum(1.0, upd_rms / hyper[2])
        return size * jnp.sqrt(s_full / own)

    def update(group_of, buf, i):
        wait_bytes(buf.at[pl.ds(0, n_dev - 1)], recv_s.at[i])
        factors = [jnp.concatenate([step_factor(buf, slot)] * len(nt), axis=1) * inv_n[m] for slot, m in enumerate(group_of)]
        for m, k in zip(group_of, factors):
            if m >= kept:
                last_factor[m - kept] = k
                continue
            w_ref = weights(m)
            k = jnp.broadcast_to(k, (8, narrow))
            k = jnp.concatenate([k] * (group // 8), axis=0)

            def apply(at, r, carry, m=m, w_ref=w_ref, k=k):
                rows = slice(r, r + group)
                w = at(w_ref)
                w[rows, :] = w[rows, :] - k * at(grad(m))[rows, :]
                return carry
            all_rows(apply, 0)

    for m in range(n_mat):
        total = jnp.zeros((8, narrow), F32)
        copies = loads(m)
        blocks = order
        if m == 0:
            for copy in copies[:2]:
                copy.wait()
            for copy in loads(1):
                copy.start()
            total = products(m, order[:1], total, True)
            blocks, copies = order[1:], copies[2:]
        for copy in copies:
            copy.wait()
        if 1 <= m < last:
            for copy in loads(m + 1):
                copy.start()
        w_copies[m].start()
        if m >= 2:
            wait_moments(m - 2)
            second_moments(m - 2)
        total = products(m, blocks, total, m > 0)
        if m == 0:
            pl.semaphore_wait(barrier, n_dev - 1)
        send_moments(m, total)

    early, late = list(range(last)), [last]
    for copy in w_copies:
        copy.wait()
    wait_moments(last - 1)
    second_moments(last - 1)
    send_scalars(early, rx_a, 0)
    sq_sum[last] = all_rows(functools.partial(square_group, last), zeros)
    wait_moments(last)
    second_moments(last)
    send_scalars(late, rx_b, 1)
    update(early, rx_a, 0)
    for m in range(n_mat):
        wait_bytes(rx_n.at[m, pl.ds(0, n_col - 1)], send_n.at[m])
        wait_bytes(rx_w.at[m, pl.ds(0, n_row - 1)], send_w.at[m])
    wait_bytes(rx_a.at[pl.ds(0, n_dev - 1)], send_s.at[0])
    wait_bytes(rx_b.at[pl.ds(0, n_dev - 1)], send_s.at[1])
    update(late, rx_b, 1)


def write_kernel(*refs):
    count = (len(refs) - 4) // 2
    srcs, (grad, factor), dsts, (stage, sem) = refs[:count], refs[count:count + 2], refs[count + 2:-2], refs[-2:]
    layers, wide, _ = srcs[3].shape
    copies = []

    def copy(src, dst):
        copies.append(pltpu.make_async_copy(src, dst, sem.at[len(copies)]))
        copies[-1].start()

    rows = wide // 2
    for i in range(layers):
        for r in (0, rows):
            copy(srcs[0].at[i, pl.ds(r, rows)], dsts[0].at[i, pl.ds(r, rows)])
    for i in (1, 2, 4, 5):
        copy(srcs[i], dsts[i])
    step = wide // 5
    for i in range(layers):
        k = factor[i]
        for r in range(0, wide, step):
            for t in range(r, r + step, 16):
                stage[i, t:t + 16, :] = srcs[3][i, t:t + 16, :] - k * grad[i, t:t + 16, :]
            copy(stage.at[i, pl.ds(r, step)], dsts[3].at[i, pl.ds(r, step)])
    for item in copies:
        item.wait()


def solution(mesh):
    n_col = mesh.shape['col']
    n_row = mesh.shape['row']
    tile_in = P(None, 'row', 'col')
    tile_out = P(None, 'col', 'row')
    lane_row = P(None, None, 'row')
    lane_col = P(None, None, 'col')
    vec_row = P(None, 'row')
    vec_col = P(None, 'col')

    def local_step(hyper_params, w_in, x_in, dy_in, row_in, col_in, w_out, x_out, dy_out, row_out, col_out):
        layers, narrow, wide = w_in.shape
        tokens = x_in.shape[1]
        n_mat = 2 * layers
        n_dev = n_col * n_row
        hbm = pl.BlockSpec(memory_space=pltpu.HBM)
        vmem = pl.BlockSpec(memory_space=pltpu.VMEM)
        smem = pl.BlockSpec(memory_space=pltpu.SMEM)
        dma = pltpu.SemaphoreType.DMA
        nr, wr = 8, 16
        swap = lambda v: jnp.swapaxes(v, 1, 2)
        sizes = (512, 512, 512, 144)
        main = narrow - LANES
        shapes = [v.shape for v in (w_out, row_in, col_in, w_out, row_out, col_out)]
        results = pl.pallas_call(
            functools.partial(stats_kernel, n_col, n_row, sizes, main),
            out_shape=tuple(pltpu.VMEM(shape, F32) for shape in shapes + [w_out.shape, (layers, 1, narrow)]),
            in_specs=[smem, hbm, hbm, hbm, vmem, vmem, hbm, hbm, hbm, vmem, vmem],
            out_specs=(vmem,) * 8,
            scratch_shapes=[
                pltpu.VMEM((n_mat - layers, wide, narrow), F32),
                pltpu.VMEM((2, tokens, narrow), jnp.bfloat16),
                pltpu.VMEM((2, wide, tokens), jnp.bfloat16),
                pltpu.VMEM((narrow - main, tokens), jnp.bfloat16),
                pltpu.VMEM((2, tokens, max(sizes)), jnp.bfloat16),
                pltpu.VMEM((wide, LANES), F32),
                pltpu.VMEM((n_mat, wide, LANES), F32),
                pltpu.VMEM((n_mat, 1, narrow), F32),
                pltpu.VMEM((n_mat, n_col, nr, LANES), F32),
                pltpu.VMEM((n_mat, n_row, wr, LANES), F32),
                pltpu.VMEM((n_dev, 3 * (n_mat - 1), 1, LANES), F32),
                pltpu.VMEM((n_dev, 3, 1, LANES), F32),
                pltpu.VMEM((n_mat, nr, LANES), F32),
                pltpu.VMEM((n_mat, wr, LANES), F32),
                dma((2,)), dma((2, len(sizes))), dma((n_mat,)),
                dma((n_mat,)), dma((n_mat,)), dma((n_mat,)), dma((n_mat,)), dma((2,)), dma((2,)),
            ],
            compiler_params=pltpu.CompilerParams(collective_id=0, has_side_effects=True, vmem_limit_bytes=38 << 20),
            name="stats",
        )(hyper_params, swap(w_in), x_in, swap(dy_in), row_in, col_in, w_out, swap(x_out), dy_out, row_out, col_out)
        w_in_new, row_in_new, col_in_new, w_out_new, row_out_new, col_out_new = pl.pallas_call(
            write_kernel,
            out_shape=tuple(pltpu.HBM(shape, F32) for shape in shapes),
            in_specs=[vmem] * 8,
            out_specs=(hbm,) * 6,
            scratch_shapes=[pltpu.VMEM(w_out.shape, F32), dma((7 * layers + 4,))],
            compiler_params=pltpu.CompilerParams(vmem_limit_bytes=10 << 20),
            name="write",
        )(*(pltpu.with_memory_space_constraint(v, pltpu.VMEM) for v in results))
        return swap(w_in_new), row_in_new, col_in_new, w_out_new, row_out_new, col_out_new

    return jax.shard_map(local_step, mesh=mesh, in_specs=(P(), tile_in, lane_row, lane_col, vec_row, vec_col, tile_out, lane_col, lane_row, vec_col, vec_row), out_specs=(tile_in, vec_row, vec_col, tile_out, vec_col, vec_row), check_vma=False)
```

```python
import functools

import jax
import jax.numpy as jnp
from jax import lax
from jax.experimental import pallas as pl
from jax.experimental.pallas import tpu as pltpu
from jax.sharding import PartitionSpec as P

EPS_ONE = 1e-30
EPS_TWO = 1e-3
MESH = pl.DeviceIdType.MESH
F32 = jnp.float32
LANES = 128


def col_tiles(width):
    return [(start, min(LANES, width - start)) for start in range(0, width, LANES)]


def stats_kernel(n_col, n_row, sizes, main, hyper, w_in, x_in, dy_in, row_in, col_in, w_out, x_out, dy_out, row_out, col_out,
                 wv_in, row_in_new, col_in_new, wv_out, row_out_new, col_out_new, last_grad, last_factor,
                 upd, a_buf, b_buf, a_t, b_t, row_acc, w_col, inv_n, rx_n, rx_w, rx_a, rx_b, old_n, old_w,
                 a_sem, b_sem, w_sem, send_n, recv_n, send_w, recv_w, send_s, recv_s):
    layers, wide, narrow = wv_in.shape
    n_mat = 2 * layers
    last = n_mat - 1
    kept = 1
    full_narrow, full_wide = narrow * n_row, wide * n_col
    n_total = float(full_narrow * full_wide)
    my_c, my_r = lax.axis_index("col"), lax.axis_index("row")
    n_dev = n_col * n_row
    me = my_c * n_row + my_r
    tiles = col_tiles(wide)
    nt = col_tiles(narrow)

    def split(start, *lengths):
        return [(start + sum(lengths[:i]), w) for i, w in enumerate(lengths)]

    order = split(0, *sizes)

    def loads(m):
        slot, layer = m % 2, m % layers
        a_src, b_src = (x_in, dy_in) if m < layers else (dy_out, x_out)
        return ([pltpu.make_async_copy(a_src.at[layer], a_buf.at[slot], a_sem.at[slot])]
                + [pltpu.make_async_copy(b_src.at[layer, pl.ds(s, w)], b_buf.at[slot, pl.ds(s, w)], b_sem.at[slot, i])
                   for i, (s, w) in enumerate(order)])

    for copy in loads(0):
        copy.start()
    barrier = pltpu.get_barrier_semaphore()
    flip = lambda v: v + 1 - 2 * lax.rem(v, 2)
    peers_c = [(n_col - 1 - my_c, 2), (lax.rem(my_c + 2, n_col), 1), (flip(my_c), 1), (my_c, 0)]
    peers_r = [(n_row - 1 - my_r, 1), (lax.rem(my_r + 2, n_row), 1), (flip(my_r), 0), (my_r, 0)]
    peers = sorted(((hops_c + hops_r, i, j) for i, (_, hops_c) in enumerate(peers_c) for j, (_, hops_r) in enumerate(peers_r)
                    if (i, j) != (3, 3)), reverse=True)
    peers = [(peers_c[i][0], peers_r[j][0]) for _, i, j in peers]
    for peer in peers:
        pl.semaphore_signal(barrier, inc=1, device_id=peer, device_id_type=MESH)

    old_n[...] = jnp.zeros_like(old_n)
    old_w[...] = jnp.zeros_like(old_w)
    for m in range(n_mat):
        rx_n[m, my_c] = jnp.zeros(rx_n.shape[2:], F32)
        rx_w[m, my_r] = jnp.zeros(rx_w.shape[2:], F32)
    for layer in range(layers):
        for m, src_n, src_w in ((layer, row_in, col_in), (layers + layer, col_out, row_out)):
            for j, (s, w) in enumerate(nt):
                old_n[m, j:j + 1, :w] = src_n[layer:layer + 1, s:s + w]
            for j, (s, w) in enumerate(tiles):
                old_w[m, j:j + 1, :w] = src_w[layer:layer + 1, s:s + w]

    w_copies = ([pltpu.make_async_copy(w_in.at[i], wv_in.at[i], w_sem.at[i]) for i in range(layers)]
                + [pltpu.make_async_copy(w_out.at[i], wv_out.at[i], w_sem.at[layers + i]) for i in range(layers)])

    def grad(m):
        return upd.at[m] if m < kept else last_grad.at[m - kept]

    def weights(m):
        return wv_in.at[m % layers] if m < layers else wv_out.at[m % layers]

    def send(buf, index, send_sem, recv_sem, peer):
        pltpu.make_async_remote_copy(src_ref=buf.at[index], dst_ref=buf.at[index], send_sem=send_sem, recv_sem=recv_sem,
                                     device_id=peer, device_id_type=MESH).start()

    def wait_bytes(ref, sem):
        pltpu.make_async_copy(ref, ref, sem).wait()

    zeros = jnp.zeros((16, narrow), F32)
    sq_sum = {}
    row_mean = {}

    group, stretch = 16, 336

    def scale_group(m, at, r, acc):
        rows = slice(r, r + group)
        g = at(grad(m))
        u = g[rows, :] * jnp.concatenate([at(w_col.at[m])[rows, :]] * len(nt), axis=1)
        g[rows, :] = u
        return acc + u * u

    def square_group(m, at, r, acc):
        v = at(weights(m))[r:r + group, :]
        return acc + v * v

    def both_group(m, at, r, accs):
        return scale_group(m, at, r, accs[0]), square_group(m, at, r, accs[1])

    def all_rows(fn, init):
        def body(i, carry):
            at = lambda ref: ref.at[pl.ds(pl.multiple_of(i * stretch, stretch), stretch)]
            for r in range(0, stretch, group):
                carry = fn(at, r, carry)
            return carry
        return lax.fori_loop(0, wide // stretch, body, init)

    def products(m, blocks, total, first):
        slot = m % 2
        if first:
            a_t[...] = a_buf[slot, :, main:].T
        for i, (s, w) in enumerate(blocks):
            block = b_buf.at[slot, pl.ds(s, w)]
            b_t[i % 2, :, :w] = block[...].T
            left = jnp.dot(block[...], a_buf[slot, :, :main], preferred_element_type=F32)
            right = jnp.dot(a_t[...], b_t[i % 2, :, :w], preferred_element_type=F32).T
            grad(m)[s:s + w, :main] = left
            grad(m)[s:s + w, main:] = right
            q = left * left
            p = right * right
            total = total + jnp.concatenate([jnp.sum(v.reshape(w // 8, 8, v.shape[1]), axis=0) for v in (q, p)], axis=1)
            for t, tw in col_tiles(main):
                p = p + q[:, t:t + tw]
            row_acc[s:s + w, :] = p
            for t, tw in tiles:
                if s < t + tw <= s + w:
                    block = row_acc[t:t + tw, :].T
                    j = t // LANES
                    rx_w[m, my_r, j:j + 1, :tw] = jnp.sum(block, axis=0, keepdims=True)
        return total

    def send_moments(m, total):
        sums = jnp.sum(total, axis=0, keepdims=True)
        for j, (t, tw) in enumerate(nt):
            rx_n[m, my_c, j:j + 1, :] = sums[:, t:t + tw]
        for c, _ in peers_c[:-1]:
            send(rx_n.at[m], my_c, send_n.at[m], recv_n.at[m], (c, my_r))
        for r, _ in peers_r[:-1]:
            send(rx_w.at[m], my_r, send_w.at[m], recv_w.at[m], (my_c, r))

    def wait_moments(m):
        wait_bytes(rx_n.at[m, pl.ds(0, n_col - 1)], recv_n.at[m])
        wait_bytes(rx_w.at[m, pl.ds(0, n_row - 1)], recv_w.at[m])

    def second_moments(m):
        beta = hyper[0]
        layer = m % layers
        sum_n = rx_n[m, 0]
        for src in range(1, n_col):
            sum_n = sum_n + rx_n[m, src]
        sum_w = rx_w[m, 0]
        for src in range(1, n_row):
            sum_w = sum_w + rx_w[m, src]
        new_n = beta * old_n[m] + (1.0 - beta) * (sum_n / full_wide + EPS_ONE)
        new_w = beta * old_w[m] + (1.0 - beta) * (sum_w / full_narrow + EPS_ONE)
        dst_n, dst_w = (row_in_new, col_in_new) if m < layers else (col_out_new, row_out_new)
        for j, (t, tw) in enumerate(nt):
            dst_n[layer:layer + 1, t:t + tw] = new_n[j:j + 1, :tw]
        for j, (t, tw) in enumerate(tiles):
            dst_w[layer:layer + 1, t:t + tw] = new_w[j:j + 1, :tw]
        v, length = (new_n, narrow) if m < layers else (new_w, wide)
        index = lax.broadcasted_iota(jnp.int32, v.shape, 0) * LANES + lax.broadcasted_iota(jnp.int32, v.shape, 1)
        mean = jnp.sum(jnp.sum(jnp.where(index < length, v, 0.0), axis=0, keepdims=True), axis=1, keepdims=True) / length
        row_mean[m] = mean
        root = jnp.sqrt(mean)
        scaled = lax.rsqrt(new_n) * root
        for j, (t, tw) in enumerate(nt):
            inv_n[m, :, t:t + tw] = scaled[j:j + 1, :]
        inv_w = lax.rsqrt(new_w)
        for j, (t, tw) in enumerate(tiles):
            w_col[m, t:t + tw, :] = jnp.broadcast_to(inv_w[j:j + 1, :tw], (LANES, tw)).T

    def send_scalars(group_of, buf, i):
        for slot, m in enumerate(group_of):
            if m in sq_sum:
                norm = all_rows(functools.partial(scale_group, m), zeros)
            else:
                norm, sq_sum[m] = all_rows(functools.partial(both_group, m), (zeros, zeros))
            norm = jnp.sum(norm, axis=0, keepdims=True) * inv_n[m] * inv_n[m]
            norm = jnp.sum(norm, axis=1, keepdims=True)
            w_sq = jnp.sum(jnp.sum(sq_sum[m], axis=0, keepdims=True), axis=1, keepdims=True)
            for row, v in enumerate((norm, w_sq, row_mean[m])):
                buf[me, 3 * slot + row] = jnp.broadcast_to(v, (1, LANES))
        for peer in peers:
            send(buf, me, send_s.at[i], recv_s.at[i], peer)

    def step_factor(buf, slot):
        norms, w_sqs, means = (buf[:, 3 * slot + row] for row in range(3))
        s_full = jnp.sum(means, axis=0) / n_dev
        own = buf[me, 3 * slot + 2]
        upd_sq = jnp.sum(norms * (s_full[None] / means), axis=0)
        w_sq = jnp.sum(w_sqs, axis=0)
        upd_rms = jnp.sqrt(upd_sq / n_total)
        w_rms = jnp.sqrt(w_sq / n_total)
        size = hyper[1] * jnp.maximum(EPS_TWO, w_rms) / jnp.maximum(1.0, upd_rms / hyper[2])
        return size * jnp.sqrt(s_full / own)

    def update(group_of, buf, i):
        wait_bytes(buf.at[pl.ds(0, n_dev - 1)], recv_s.at[i])
        factors = [jnp.concatenate([step_factor(buf, slot)] * len(nt), axis=1) * inv_n[m] for slot, m in enumerate(group_of)]
        for m, k in zip(group_of, factors):
            if m >= kept:
                last_factor[m - kept] = k
                continue
            w_ref = weights(m)
            k = jnp.broadcast_to(k, (8, narrow))
            k = jnp.concatenate([k] * (group // 8), axis=0)

            def apply(at, r, carry, m=m, w_ref=w_ref, k=k):
                rows = slice(r, r + group)
                w = at(w_ref)
                w[rows, :] = w[rows, :] - k * at(grad(m))[rows, :]
                return carry
            all_rows(apply, 0)

    for m in range(n_mat):
        total = jnp.zeros((8, narrow), F32)
        copies = loads(m)
        blocks = order
        if m == 0:
            for copy in copies[:2]:
                copy.wait()
            for copy in loads(1):
                copy.start()
            total = products(m, order[:1], total, True)
            blocks, copies = order[1:], copies[2:]
        for copy in copies:
            copy.wait()
        if 1 <= m < last:
            for copy in loads(m + 1):
                copy.start()
        w_copies[m].start()
        if m >= 2:
            wait_moments(m - 2)
            second_moments(m - 2)
        total = products(m, blocks, total, m > 0)
        if m == 0:
            pl.semaphore_wait(barrier, n_dev - 1)
        send_moments(m, total)

    early, late = list(range(last)), [last]
    for copy in w_copies:
        copy.wait()
    wait_moments(last - 1)
    second_moments(last - 1)
    send_scalars(early, rx_a, 0)
    sq_sum[last] = all_rows(functools.partial(square_group, last), zeros)
    wait_moments(last)
    second_moments(last)
    send_scalars(late, rx_b, 1)
    update(early, rx_a, 0)
    for m in range(n_mat):
        wait_bytes(rx_n.at[m, pl.ds(0, n_col - 1)], send_n.at[m])
        wait_bytes(rx_w.at[m, pl.ds(0, n_row - 1)], send_w.at[m])
    wait_bytes(rx_a.at[pl.ds(0, n_dev - 1)], send_s.at[0])
    wait_bytes(rx_b.at[pl.ds(0, n_dev - 1)], send_s.at[1])
    update(late, rx_b, 1)


def write_kernel(*refs):
    srcs, (_, factor), dsts, (grad, sem) = refs[:6], refs[6:8], refs[8:14], refs[14:]
    layers, wide, _ = srcs[3].shape
    copies = []

    def copy(src, dst):
        copies.append(pltpu.make_async_copy(src, dst, sem.at[len(copies)]))
        copies[-1].start()

    rows = wide // 2
    for r in (0, rows):
        copy(srcs[0].at[0, pl.ds(r, rows)], dsts[0].at[0, pl.ds(r, rows)])
    for i in (1, 2, 4, 5):
        copy(srcs[i], dsts[i])
    step = wide // 5
    for m in range(1, 2 * layers):
        k = factor[m - 1]
        src, dst = (srcs[0].at[m], dsts[0].at[m]) if m < layers else (srcs[3].at[m - layers], dsts[3].at[m - layers])
        for r in range(0, wide, step):
            for t in range(r, r + step, 16):
                grad[m - 1, t:t + 16, :] = src[t:t + 16, :] - k * grad[m - 1, t:t + 16, :]
            copy(grad.at[m - 1, pl.ds(r, step)], dst.at[pl.ds(r, step)])
    for item in copies:
        item.wait()


def solution(mesh):
    n_col = mesh.shape['col']
    n_row = mesh.shape['row']
    tile_in = P(None, 'row', 'col')
    tile_out = P(None, 'col', 'row')
    lane_row = P(None, None, 'row')
    lane_col = P(None, None, 'col')
    vec_row = P(None, 'row')
    vec_col = P(None, 'col')

    def local_step(hyper_params, w_in, x_in, dy_in, row_in, col_in, w_out, x_out, dy_out, row_out, col_out):
        layers, narrow, wide = w_in.shape
        tokens = x_in.shape[1]
        n_mat = 2 * layers
        n_dev = n_col * n_row
        hbm = pl.BlockSpec(memory_space=pltpu.HBM)
        vmem = pl.BlockSpec(memory_space=pltpu.VMEM)
        smem = pl.BlockSpec(memory_space=pltpu.SMEM)
        dma = pltpu.SemaphoreType.DMA
        nr, wr = 8, 16
        swap = lambda v: jnp.swapaxes(v, 1, 2)
        sizes = (512, 512, 512, 144)
        main = narrow - LANES
        shapes = [v.shape for v in (w_out, row_in, col_in, w_out, row_out, col_out)]
        results = pl.pallas_call(
            functools.partial(stats_kernel, n_col, n_row, sizes, main),
            out_shape=tuple(pltpu.VMEM(shape, F32) for shape in shapes + [(n_mat - 1, wide, narrow), (n_mat - 1, 1, narrow)]),
            in_specs=[smem, hbm, hbm, hbm, vmem, vmem, hbm, hbm, hbm, vmem, vmem],
            out_specs=(vmem,) * 8,
            scratch_shapes=[
                pltpu.VMEM((1, wide, narrow), F32),
                pltpu.VMEM((2, tokens, narrow), jnp.bfloat16),
                pltpu.VMEM((2, wide, tokens), jnp.bfloat16),
                pltpu.VMEM((narrow - main, tokens), jnp.bfloat16),
                pltpu.VMEM((2, tokens, max(sizes)), jnp.bfloat16),
                pltpu.VMEM((wide, LANES), F32),
                pltpu.VMEM((n_mat, wide, LANES), F32),
                pltpu.VMEM((n_mat, 1, narrow), F32),
                pltpu.VMEM((n_mat, n_col, nr, LANES), F32),
                pltpu.VMEM((n_mat, n_row, wr, LANES), F32),
                pltpu.VMEM((n_dev, 3 * (n_mat - 1), 1, LANES), F32),
                pltpu.VMEM((n_dev, 3, 1, LANES), F32),
                pltpu.VMEM((n_mat, nr, LANES), F32),
                pltpu.VMEM((n_mat, wr, LANES), F32),
                dma((2,)), dma((2, len(sizes))), dma((n_mat,)),
                dma((n_mat,)), dma((n_mat,)), dma((n_mat,)), dma((n_mat,)), dma((2,)), dma((2,)),
            ],
            compiler_params=pltpu.CompilerParams(collective_id=0, has_side_effects=True, vmem_limit_bytes=34 << 20),
            name="stats",
        )(hyper_params, swap(w_in), x_in, swap(dy_in), row_in, col_in, w_out, swap(x_out), dy_out, row_out, col_out)
        w_in_new, row_in_new, col_in_new, w_out_new, row_out_new, col_out_new, _ = pl.pallas_call(
            write_kernel,
            out_shape=tuple(pltpu.HBM(shape, F32) for shape in shapes) + (pltpu.VMEM((n_mat - 1, wide, narrow), F32),),
            in_specs=[vmem] * 8,
            out_specs=(hbm,) * 6 + (vmem,),
            scratch_shapes=[dma((5 * n_mat + 1,))],
            input_output_aliases={6: 6},
            compiler_params=pltpu.CompilerParams(vmem_limit_bytes=1 << 20),
            name="write",
        )(*(pltpu.with_memory_space_constraint(v, pltpu.VMEM) for v in results))
        return swap(w_in_new), row_in_new, col_in_new, w_out_new, row_out_new, col_out_new

    return jax.shard_map(local_step, mesh=mesh, in_specs=(P(), tile_in, lane_row, lane_col, vec_row, vec_col, tile_out, lane_col, lane_row, vec_col, vec_row), out_specs=(tile_in, vec_row, vec_col, tile_out, vec_col, vec_row), check_vma=False)
```
